128 devices in a mesh: band: 16 (over z, x), coef: 8 (over y, core).
Axes of the slice: x: 4, y: 4, z: 4, core: 2. Of those that a mesh axis runs over, the one named last changes fastest.
Arguments:
- coeffs: float32 [1024, 262144], P('band', 'coef'), may hold values from -320 to 320
- ref_block: float32 [1024, 262144], P('band', 'coef'), may hold values from -0.01171875 to 0.01171875
- index_map: int32 [262144], P('coef'), may hold values from 0 to 32767, as said below
- band_group: int32 [1024], P('band'), may hold values from 0 to 15
Outputs:
- ortho: float32 [1024, 262144], P('band', 'coef')
- band_residual: float32 [1024], P('band')
- group_residual: float32 [16], replicated
The draws below stay inside these ranges and needn't reach their ends.
Inputs may be any that keep to these rules, and one draw needn't show every extreme that they name: Within each aligned slab of 32768 coefficients, index_map holds every number of 0 to 32767 once.
All inputs are finite; a program needn't handle non-finite values.
Results may differ from the reference program's by a relative error of at most 0.000098.
Values sent between devices are 32-bit elements; how exact they have to be, the bound alone decides.
A program may use at most 192 MiB of HBM per device.

```python
import math
import jax
import jax.numpy as jnp
from jax import lax

NB = 1024
NG = 262144
NGROUPS = 16
GS = 32768


def shared_basis(key):
    base = jax.random.fold_in(key, 11)
    basis = jnp.clip(jax.random.normal(base, (NB, NG), jnp.float32), -6.0, 6.0)
    return basis


def slab_order(key):
    base = jax.random.fold_in(key, 23)
    slabs = NG // GS
    starts = jnp.arange(slabs)
    keys = jax.vmap(lambda number: jax.random.fold_in(base, number))(starts)
    return jax.vmap(lambda single: jax.random.permutation(single, GS))(keys).astype(jnp.int32)


def draw_coeffs(key, part):
    basis = shared_basis(key)
    mixing = jax.random.uniform(jax.random.fold_in(key, 31), (NB,), jnp.float32, 0.3, 0.6)
    scales = jnp.exp(jax.random.uniform(jax.random.fold_in(key, 37), (NB,), jnp.float32, 0.0, math.log(10.0)))
    mixed = basis + mixing[:, None] * jnp.roll(basis, 1, axis=0)
    return (scales[:, None] * mixed).astype(jnp.float32)


def draw_ref_block(key, part):
    basis = shared_basis(key)
    order = slab_order(key)
    slabs = NG // GS
    shaped = basis.reshape(NB, slabs, GS)
    moved = jnp.take_along_axis(shaped, order[None, :, :], axis=2).reshape(NB, NG)
    return (moved / math.sqrt(NG)).astype(jnp.float32)


def draw_index_map(key, part):
    return slab_order(key).reshape(NG).astype(jnp.int32)


def touch_ends(values, own_key, least, top_value):
    longest = values.shape.index(max(values.shape))
    spots = []
    for shift in (0, 1):
        where = [jax.random.randint(jax.random.fold_in(own_key, axis), (), 0, length) for axis, length in enumerate(values.shape)]
        where[longest] = (where[longest] + shift) % values.shape[longest]
        spots.append(tuple(where))
    return values.at[spots[0]].set(least).at[spots[1]].set(top_value)


def setup_inputs(seed: int = 0) -> dict:
    streams_of = jax.random.split(jax.random.key(seed), 5)
    coeffs = draw_coeffs(jax.random.fold_in(streams_of[4], 71), 0)
    ref_block = draw_ref_block(jax.random.fold_in(streams_of[4], 71), 0)
    index_map = draw_index_map(jax.random.fold_in(streams_of[4], 71), 0)
    band_group = touch_ends(jax.random.randint(streams_of[3], (NB,), 0, NGROUPS), jax.random.fold_in(streams_of[3], 1), 0, NGROUPS - 1).astype(jnp.int32)
    return dict(coeffs=coeffs, ref_block=ref_block, index_map=index_map, band_group=band_group)


def reference(coeffs, ref_block, index_map, band_group):
    margin = jnp.dot(coeffs.astype(jnp.float32), coeffs.T.astype(jnp.float32), precision=lax.Precision.HIGHEST, preferred_element_type=jnp.float32)
    factor = jnp.linalg.cholesky(margin)
    ortho = lax.linalg.triangular_solve(factor, coeffs, left_side=True, lower=True)
    slabs = NG // GS
    shaped = ortho.reshape(NB, slabs, GS)
    order = index_map.reshape(slabs, GS).astype(jnp.int32)
    aligned = jnp.take_along_axis(shaped, order[None, :, :], axis=2).reshape(NB, NG)
    squares = lax.optimization_barrier(jnp.sum((aligned - ref_block) ** 2, axis=1))
    band_residual = jnp.sqrt(squares + 1e-06)
    group_residual = jax.ops.segment_sum(band_residual, band_group, num_segments=NGROUPS) * (NGROUPS / NB)
    return (ortho, band_residual, group_residual.astype(jnp.float32))
```

```python
import functools
import jax
import jax.numpy as jnp
from jax import lax
from jax.experimental import pallas as pl
from jax.experimental.pallas import tpu as pltpu

BLK = 128
PAN = 8
F32 = jnp.float32
BF = jnp.bfloat16


def split(x):
    hi = x.astype(BF)
    return hi, (x - hi.astype(F32)).astype(BF)


def dot3(ah, al, bh, bl, dims):
    d = functools.partial(lax.dot_general, dimension_numbers=(dims, ((), ())), preferred_element_type=F32)
    return d(ah, bh) + (d(ah, bl) + d(al, bh))


NN = ((1,), (0,))
NT = ((1,), (1,))


def lanes_of(x, lane):
    return jnp.take_along_axis(x, jnp.full(x.shape, lane, jnp.int32), axis=1)


def row_of(x, j):
    return jnp.broadcast_to(x[j : j + 1, :], (PAN, BLK))


def rows_sum(cols, rows):
    parts = [c * r for c, r in zip(cols, rows)]
    while len(parts) > 1:
        parts = [parts[i] + parts[i + 1] for i in range(0, len(parts), 2)]
    return parts[0]


def diag_inverse(a_ref, w_ref, m_ref):
    sub = lax.broadcasted_iota(jnp.int32, (PAN, BLK), 0)
    r_i = lax.broadcasted_iota(jnp.int32, (BLK, BLK), 0)
    c_i = lax.broadcasted_iota(jnp.int32, (BLK, BLK), 1)
    w_ref[...] = (r_i == c_i).astype(F32)

    def body(p, carry):
        x, *cols = carry
        base = pl.multiple_of(p * PAN, PAN)
        nxt = pl.multiple_of(jnp.minimum(base + PAN, BLK - PAN), PAN)
        fwd = w_ref[pl.ds(base, PAN), :]
        kw = fwd
        scale = jnp.zeros((PAN, BLK), F32)
        for j in range(PAN):
            d = row_of(cols[j], j)
            r = 1.0 / d
            f = cols[j] * r
            isj = sub == j
            for m in range(j + 1, PAN):
                b = row_of(cols[m], j)
                cols[m] = jnp.where(isj, b * r, cols[m] - f * b)
            b = row_of(x, j)
            x = jnp.where(isj, b * r, x - f * b)
            b = row_of(kw, j)
            kw = jnp.where(isj, b * r, kw - f * b)
            if j < PAN - 1:
                fwd = jnp.where(sub > j, fwd - f * row_of(fwd, j), fwd)
            scale = jnp.where(isj, lax.rsqrt(d), scale)
        m_ref[pl.ds(base, PAN), :] = fwd * scale
        xb = [row_of(x, m) for m in range(PAN)]
        kb = [row_of(kw, m) for m in range(PAN)]
        an = a_ref[pl.ds(nxt, PAN), :]
        xn = an - rows_sum([lanes_of(an, base + m) for m in range(PAN)], xb)
        new_cols = [lanes_of(xn, nxt + m) for m in range(PAN)]
        for s in range(0, BLK, PAN):
            a = a_ref[s : s + PAN, :]
            am = [lanes_of(a, base + m) for m in range(PAN)]
            a_ref[s : s + PAN, :] = a - rows_sum(am, xb)
            w_ref[s : s + PAN, :] = w_ref[s : s + PAN, :] - rows_sum(am, kb)
        return (xn, *new_cols)

    x0 = a_ref[0:PAN, :]
    lax.fori_loop(0, BLK // PAN, body, (x0, *[lanes_of(x0, m) for m in range(PAN)]))


def solve_kernel(g_ref, c_ref, y_ref, a_ref, w_ref, m_ref, lh_ref, ll_ref, yh_ref, yl_ref):
    n = g_ref.shape[0]
    for k in range(n // BLK):
        lo, hi = k * BLK, (k + 1) * BLK
        s = g_ref[lo:, lo:hi]
        if k:
            s = s - dot3(lh_ref[lo:, :lo], ll_ref[lo:, :lo], lh_ref[lo:hi, :lo], ll_ref[lo:hi, :lo], NT)
        a_ref[...] = s[:BLK]
        diag_inverse(a_ref, w_ref, m_ref)
        mh, ml = split(m_ref[...])
        if hi < n:
            sh, sl = split(s[BLK:])
            lkh, lkl = split(dot3(sh, sl, mh, ml, NT))
            lh_ref[hi:, lo:hi] = lkh
            ll_ref[hi:, lo:hi] = lkl
        z = c_ref[lo:hi, :]
        if k:
            z = z - dot3(lh_ref[lo:hi, :lo], ll_ref[lo:hi, :lo], yh_ref[:lo, :], yl_ref[:lo, :], NN)
        zh, zl = split(z)
        y = dot3(mh, ml, zh, zl, NN)
        y_ref[lo:hi, :] = y
        if hi < n:
            yh, yl = split(y)
            yh_ref[lo:hi, :] = yh
            yl_ref[lo:hi, :] = yl


def solve(g, c):
    n, w = c.shape
    return pl.pallas_call(
        solve_kernel,
        out_shape=jax.ShapeDtypeStruct((n, w), F32),
        in_specs=[pl.BlockSpec(memory_space=pltpu.VMEM)] * 2,
        out_specs=pl.BlockSpec(memory_space=pltpu.VMEM),
        scratch_shapes=[pltpu.VMEM((BLK, BLK), F32)] * 3
        + [pltpu.VMEM((n, n), BF)] * 2
        + [pltpu.VMEM((n, w), BF)] * 2,
        compiler_params=pltpu.CompilerParams(vmem_limit_bytes=60 * 2**20),
        name="solve",
    )(g, c)


def gram_kernel(c_ref, g_ref, h_ref, l_ref):
    n = c_ref.shape[0]
    b = 256
    for i in range(n // b):
        h, l = split(c_ref[i * b : (i + 1) * b, :])
        h_ref[i * b : (i + 1) * b, :] = h
        l_ref[i * b : (i + 1) * b, :] = l
        e = (i + 1) * b
        g_ref[i * b : e, :e] = dot3(h, l, h_ref[:e, :], l_ref[:e, :], NT)
        if e < n:
            g_ref[i * b : e, e:] = jnp.zeros((b, n - e), F32)


def gram(c):
    n, w = c.shape
    return pl.pallas_call(
        gram_kernel,
        out_shape=jax.ShapeDtypeStruct((n, n), F32),
        in_specs=[pl.BlockSpec(memory_space=pltpu.VMEM)],
        out_specs=pl.BlockSpec(memory_space=pltpu.VMEM),
        scratch_shapes=[pltpu.VMEM((n, w), BF)] * 2,
        compiler_params=pltpu.CompilerParams(vmem_limit_bytes=60 * 2**20),
        name="gram",
    )(c)


CH = 2048


def scatter_kernel(idx_ref, r_ref, o_ref):
    def body(i, _):
        base = i * 16
        for u in range(16):
            o_ref[pl.ds(idx_ref[base + u], 1), :] = r_ref[pl.ds(base + u, 1), :]
        return 0

    lax.fori_loop(0, CH // 16, body, 0)


def scatter_rows(idx, rows):
    n, w = rows.shape
    return pl.pallas_call(
        scatter_kernel,
        grid=(n // CH,),
        out_shape=jax.ShapeDtypeStruct((n, w), F32),
        in_specs=[
            pl.BlockSpec((CH,), lambda i: (i,), memory_space=pltpu.SMEM),
            pl.BlockSpec((CH, w), lambda i: (i, 0)),
        ],
        out_specs=pl.BlockSpec((n, w), lambda i: (0, 0)),
        compiler_params=pltpu.CompilerParams(vmem_limit_bytes=60 * 2**20),
        name="scatter",
    )(idx, rows)


from jax.sharding import PartitionSpec as P

NB = 1024
NGROUPS = 16


def copy_for_each(x, axis):
    copies = jnp.broadcast_to(x, (lax.axis_size(axis), *x.shape))
    return lax.all_to_all(copies, axis, split_axis=0, concat_axis=0, tiled=True)


def of_everyone(x, axis):
    return copy_for_each(x, axis).sum(axis=0)


def local(coeffs, ref_block, index_map, band_group):
    bands, width = coeffs.shape
    parts = lax.axis_size("band")
    part = width // parts
    blocks = coeffs.reshape(bands, parts, part).transpose(1, 0, 2)
    columns = lax.all_to_all(blocks, "band", split_axis=0, concat_axis=0, tiled=True)
    columns = columns.reshape(parts * bands, part)
    moved = scatter_rows(index_map, ref_block.T).T
    margin = lax.psum(gram(columns), ("band", "coef"))
    ortho_cols = solve(margin, columns).reshape(parts, bands, part)
    back = lax.all_to_all(ortho_cols, "band", split_axis=0, concat_axis=0, tiled=True)
    ortho = back.transpose(1, 0, 2).reshape(bands, width)
    squares = jnp.sum((ortho - moved) ** 2, axis=1)
    group_range = jnp.arange(NGROUPS, dtype=jnp.int32)
    totals = of_everyone(squares, "coef")
    band_residual = jnp.sqrt(totals + 1e-06)
    onehot = (band_group[:, None] == group_range[None, :]).astype(F32)
    terms = jnp.dot(
        band_residual, onehot, precision=lax.Precision.HIGHEST, preferred_element_type=F32
    )
    group_residual = of_everyone(terms, "band") * (NGROUPS / NB)
    return (ortho, band_residual, group_residual)


def solution(mesh):
    return jax.shard_map(
        local,
        mesh=mesh,
        in_specs=(P("band", "coef"), P("band", "coef"), P("coef"), P("band")),
        out_specs=(P("band", "coef"), P("band"), P()),
        check_vma=False,
    )
```

```python
import functools
import jax
import jax.numpy as jnp
from jax import lax
from jax.experimental import pallas as pl
from jax.experimental.pallas import tpu as pltpu
from jax.sharding import PartitionSpec as P

BLK = 128
PAN = 8
F32 = jnp.float32
BF = jnp.bfloat16


def split(x):
    hi = x.astype(BF)
    return hi, (x - hi.astype(F32)).astype(BF)


def dot3(ah, al, bh, bl, dims):
    d = functools.partial(lax.dot_general, dimension_numbers=(dims, ((), ())), preferred_element_type=F32)
    return d(ah, bh) + (d(ah, bl) + d(al, bh))


NN = ((1,), (0,))
NT = ((1,), (1,))


def lanes_of(x, lane):
    return jnp.take_along_axis(x, jnp.full(x.shape, lane, jnp.int32), axis=1)


def row_of(x, j):
    return jnp.broadcast_to(x[j : j + 1, :], (PAN, BLK))


def rows_sum(cols, rows):
    parts = [c * r for c, r in zip(cols, rows)]
    while len(parts) > 1:
        parts = [parts[i] + parts[i + 1] for i in range(0, len(parts), 2)]
    return parts[0]


def diag_inverse(a_ref, w_ref, m_ref):
    sub = lax.broadcasted_iota(jnp.int32, (PAN, BLK), 0)
    r_i = lax.broadcasted_iota(jnp.int32, (BLK, BLK), 0)
    c_i = lax.broadcasted_iota(jnp.int32, (BLK, BLK), 1)
    w_ref[...] = (r_i == c_i).astype(F32)

    def body(p, carry):
        x, *cols = carry
        base = pl.multiple_of(p * PAN, PAN)
        nxt = pl.multiple_of(jnp.minimum(base + PAN, BLK - PAN), PAN)
        fwd = w_ref[pl.ds(base, PAN), :]
        kw = fwd
        scale = jnp.zeros((PAN, BLK), F32)
        for j in range(PAN):
            d = row_of(cols[j], j)
            r = 1.0 / d
            f = cols[j] * r
            isj = sub == j
            for m in range(j + 1, PAN):
                b = row_of(cols[m], j)
                cols[m] = jnp.where(isj, b * r, cols[m] - f * b)
            b = row_of(x, j)
            x = jnp.where(isj, b * r, x - f * b)
            b = row_of(kw, j)
            kw = jnp.where(isj, b * r, kw - f * b)
            if j < PAN - 1:
                fwd = jnp.where(sub > j, fwd - f * row_of(fwd, j), fwd)
            scale = jnp.where(isj, lax.rsqrt(d), scale)
        m_ref[pl.ds(base, PAN), :] = fwd * scale
        xb = [row_of(x, m) for m in range(PAN)]
        kb = [row_of(kw, m) for m in range(PAN)]
        an = a_ref[pl.ds(nxt, PAN), :]
        xn = an - rows_sum([lanes_of(an, base + m) for m in range(PAN)], xb)
        new_cols = [lanes_of(xn, nxt + m) for m in range(PAN)]
        for s in range(0, BLK, PAN):
            a = a_ref[s : s + PAN, :]
            am = [lanes_of(a, base + m) for m in range(PAN)]
            a_ref[s : s + PAN, :] = a - rows_sum(am, xb)
            w_ref[s : s + PAN, :] = w_ref[s : s + PAN, :] - rows_sum(am, kb)
        return (xn, *new_cols)

    x0 = a_ref[0:PAN, :]
    lax.fori_loop(0, BLK // PAN, body, (x0, *[lanes_of(x0, m) for m in range(PAN)]))


MESH = pl.DeviceIdType.MESH
NB = 1024
NGROUPS = 16
NBLK = NB // BLK
TILES = NBLK * (NBLK + 1) // 2
ANY = pl.BlockSpec(memory_space=pl.ANY)


def tile_row(i, j):
    return (i * (i + 1) // 2 + j) * BLK


def place():
    band, coef = lax.axis_index("band"), lax.axis_index("coef")
    return band, coef, dict(z=band // 4, x=band % 4, y=coef // 2, core=coef % 2)


def peer_on(pos, dim, value):
    p = dict(pos)
    p[dim] = value
    return (p["z"] * 4 + p["x"], p["y"] * 2 + p["core"])


def send(src, dst, ssem, rsem, device):
    copy = pltpu.make_async_remote_copy(
        src_ref=src, dst_ref=dst, send_sem=ssem, recv_sem=rsem, device_id=device, device_id_type=MESH
    )
    copy.start()
    return copy


ORDERS = (("z", "x", "y"), ("x", "y", "z"), ("y", "z", "x"))
RING = 4
HALF = TILES * BLK // 2
PART = HALF // 3
Q1 = PART // RING
Q2 = Q1 // RING


def reduce_kernel(g_ref, o_ref, half_ref, b1_ref, a1_ref, b2_ref, b3_ref, csem, rsem, ssem):
    _, _, pos = place()
    partner = peer_on(pos, "core", 1 - pos["core"])
    peers = [partner] + [
        peer_on(pos, d, lax.rem(pos[d] + r, RING)) for d in ("z", "x", "y") for r in range(1, RING)
    ]
    barrier = pltpu.get_barrier_semaphore()
    for p in peers:
        pl.semaphore_signal(barrier, inc=1, device_id=p, device_id_type=MESH)
    pl.semaphore_wait(barrier, len(peers))

    core = pos["core"]
    mine = pl.multiple_of(core * HALF, PART)
    other = pl.multiple_of((1 - core) * HALF, PART)
    cs = [
        send(
            g_ref.at[pl.ds(pl.multiple_of(other + part * PART, PART), PART)],
            half_ref.at[part],
            csem.at[part],
            csem.at[3 + part],
            partner,
        )
        for part in range(3)
    ]
    c1 = []
    for part, (d1, _, _) in enumerate(ORDERS):
        cs[part].wait_recv()
        half_ref[part] = half_ref[part] + g_ref[pl.ds(pl.multiple_of(mine + part * PART, PART), PART), :]
        for r in (2, 1, 3):
            to = lax.rem(pos[d1] + r, RING)
            c1.append(
                send(
                    half_ref.at[part, pl.ds(pl.multiple_of(to * Q1, Q1), Q1)],
                    b1_ref.at[part, r - 1],
                    ssem.at[0, part, r - 1],
                    rsem.at[0, part, r - 1],
                    peer_on(pos, d1, to),
                )
            )
    c2 = []
    for part, (d1, d2, _) in enumerate(ORDERS):
        for c in c1[3 * part : 3 * part + 3]:
            c.wait_recv()
        own = half_ref[part, pl.ds(pl.multiple_of(pos[d1] * Q1, Q1), Q1), :]
        a1_ref[part] = own + b1_ref[part, 0] + (b1_ref[part, 1] + b1_ref[part, 2])
        for r in (2, 1, 3):
            to = lax.rem(pos[d2] + r, RING)
            c2.append(
                send(
                    a1_ref.at[part, pl.ds(pl.multiple_of(to * Q2, Q2), Q2)],
                    b2_ref.at[part, r - 1],
                    ssem.at[1, part, r - 1],
                    rsem.at[1, part, r - 1],
                    peer_on(pos, d2, to),
                )
            )
    c3 = []
    for part, (d1, d2, d3) in enumerate(ORDERS):
        for c in c2[3 * part : 3 * part + 3]:
            c.wait_recv()
        own = a1_ref[part, pl.ds(pl.multiple_of(pos[d2] * Q2, Q2), Q2), :]
        b3_ref[part, pos[d3]] = own + b2_ref[part, 0] + (b2_ref[part, 1] + b2_ref[part, 2])
        for r in (2, 1, 3):
            to = lax.rem(pos[d3] + r, RING)
            c3.append(
                send(
                    b3_ref.at[part, pos[d3]],
                    b3_ref.at[part, pos[d3]],
                    ssem.at[2, part, r - 1],
                    rsem.at[2, part, r - 1],
                    peer_on(pos, d3, to),
                )
            )
    c4 = []
    for part, (d1, d2, d3) in enumerate(ORDERS):
        for c in c3[3 * part : 3 * part + 3]:
            c.wait_recv()
        start = pl.multiple_of(mine + part * PART + pos[d1] * Q1 + pos[d2] * Q2, Q2)
        o_ref[pl.ds(start, Q2), :] = (b3_ref[part, 0] + b3_ref[part, 1]) + (b3_ref[part, 2] + b3_ref[part, 3])
        here = o_ref.at[pl.ds(start, Q2)]
        for r in (2, 1, 3):
            to = lax.rem(pos[d2] + r, RING)
            c4.append(send(here, here, ssem.at[3, part, r - 1], rsem.at[3, part, r - 1], peer_on(pos, d2, to)))
    c5 = []
    for part, (d1, d2, d3) in enumerate(ORDERS):
        for c in c4[3 * part : 3 * part + 3]:
            c.wait_recv()
        here = o_ref.at[pl.ds(pl.multiple_of(mine + part * PART + pos[d1] * Q1, Q2), Q1)]
        for r in (2, 1, 3):
            to = lax.rem(pos[d1] + r, RING)
            c5.append(send(here, here, ssem.at[4, part, r - 1], rsem.at[4, part, r - 1], peer_on(pos, d1, to)))
    c6 = []
    for part, (d1, d2, d3) in enumerate(ORDERS):
        for c in c5[3 * part : 3 * part + 3]:
            c.wait_recv()
        here = o_ref.at[pl.ds(pl.multiple_of(mine + part * PART, PART), PART)]
        c6.append(send(here, here, csem.at[6 + part], csem.at[9 + part], partner))
    for c in c6:
        c.wait_recv()
    for c in cs + c1 + c2 + c3 + c4 + c5 + c6:
        c.wait_send()


def reduce_all(g):
    return pl.pallas_call(
        reduce_kernel,
        out_shape=jax.ShapeDtypeStruct(g.shape, F32),
        in_specs=[pl.BlockSpec(memory_space=pltpu.VMEM)],
        out_specs=pl.BlockSpec(memory_space=pltpu.VMEM),
        scratch_shapes=[
            pltpu.VMEM((3, PART, BLK), F32),
            pltpu.VMEM((3, RING - 1, Q1, BLK), F32),
            pltpu.VMEM((3, Q1, BLK), F32),
            pltpu.VMEM((3, RING - 1, Q2, BLK), F32),
            pltpu.VMEM((3, RING, Q2, BLK), F32),
            pltpu.SemaphoreType.DMA((12,)),
            pltpu.SemaphoreType.DMA((5, 3, RING - 1)),
            pltpu.SemaphoreType.DMA((5, 3, RING - 1)),
        ],
        compiler_params=pltpu.CompilerParams(collective_id=0, has_side_effects=True, vmem_limit_bytes=60 * 2**20),
        name="reduce_all",
    )(g)


def solve_kernel(g_ref, c_ref, y_ref, a_ref, w_ref, m_ref, lh_ref, ll_ref, yh_ref, yl_ref, z_ref, csem, ysem):
    n = c_ref.shape[0]
    steps = n // BLK
    loads = []
    for k in range(steps):
        rows = pl.ds(k * BLK, BLK)
        loads.append(pltpu.make_async_copy(c_ref.at[rows], z_ref.at[rows], csem.at[k]))
        loads[-1].start()
    stores = []
    for k in range(steps):
        lo, hi = k * BLK, (k + 1) * BLK
        s = jnp.concatenate([g_ref[tile_row(i, k) : tile_row(i, k) + BLK, :] for i in range(k, steps)], axis=0)
        if k:
            s = s - dot3(lh_ref[lo:, :lo], ll_ref[lo:, :lo], lh_ref[lo:hi, :lo], ll_ref[lo:hi, :lo], NT)
        a_ref[...] = s[:BLK]
        diag_inverse(a_ref, w_ref, m_ref)
        mh, ml = split(m_ref[...])
        if hi < n:
            sh, sl = split(s[BLK:])
            lkh, lkl = split(dot3(sh, sl, mh, ml, NT))
            lh_ref[hi:, lo:hi] = lkh
            ll_ref[hi:, lo:hi] = lkl
        loads[k].wait()
        z = z_ref[lo:hi, :]
        if k:
            z = z - dot3(lh_ref[lo:hi, :lo], ll_ref[lo:hi, :lo], yh_ref[:lo, :], yl_ref[:lo, :], NN)
        zh, zl = split(z)
        y = dot3(mh, ml, zh, zl, NN)
        z_ref[lo:hi, :] = y
        rows = pl.ds(lo, BLK)
        stores.append(pltpu.make_async_copy(z_ref.at[rows], y_ref.at[rows], ysem.at[k]))
        stores[-1].start()
        if hi < n:
            yh, yl = split(y)
            yh_ref[lo:hi, :] = yh
            yl_ref[lo:hi, :] = yl
    for c in stores:
        c.wait()


def solve(g, c):
    n, w = c.shape
    return pl.pallas_call(
        solve_kernel,
        out_shape=jax.ShapeDtypeStruct((n, w), F32),
        in_specs=[pl.BlockSpec(memory_space=pltpu.VMEM), ANY],
        out_specs=ANY,
        scratch_shapes=[pltpu.VMEM((BLK, BLK), F32)] * 3
        + [pltpu.VMEM((n, n), BF)] * 2
        + [pltpu.VMEM((n, w), BF)] * 2
        + [pltpu.VMEM((n, w), F32), pltpu.SemaphoreType.DMA((n // BLK,)), pltpu.SemaphoreType.DMA((n // BLK,))],
        compiler_params=pltpu.CompilerParams(vmem_limit_bytes=60 * 2**20),
        name="solve",
    )(g, c)


GB = 256


def gram_kernel(c_ref, g_ref, x_ref, h_ref, l_ref, sem):
    n = c_ref.shape[0]
    loads = []
    for i in range(n // GB):
        rows = pl.ds(i * GB, GB)
        loads.append(pltpu.make_async_copy(c_ref.at[rows], x_ref.at[rows], sem.at[i]))
        loads[-1].start()
    for i in range(n // GB):
        lo, e = i * GB, (i + 1) * GB
        loads[i].wait()
        h, l = split(x_ref[lo:e, :])
        h_ref[lo:e, :] = h
        l_ref[lo:e, :] = l
        g = dot3(h, l, h_ref[:e, :], l_ref[:e, :], NT)
        for bi in range(lo // BLK, e // BLK):
            for bj in range(bi + 1):
                t = tile_row(bi, bj)
                r = bi * BLK - lo
                g_ref[t : t + BLK, :] = g[r : r + BLK, bj * BLK : (bj + 1) * BLK]


def gram(c):
    n, w = c.shape
    return pl.pallas_call(
        gram_kernel,
        out_shape=jax.ShapeDtypeStruct((TILES * BLK, BLK), F32),
        in_specs=[ANY],
        out_specs=pl.BlockSpec(memory_space=pltpu.VMEM),
        scratch_shapes=[
            pltpu.VMEM((n, w), F32),
            pltpu.VMEM((n, w), BF),
            pltpu.VMEM((n, w), BF),
            pltpu.SemaphoreType.DMA((n // GB,)),
        ],
        compiler_params=pltpu.CompilerParams(vmem_limit_bytes=60 * 2**20),
        name="gram",
    )(c)


CH = 2048


def scatter_kernel(idx_ref, r_ref, o_ref, rows_ref, to_ref):
    rows_ref[...] = r_ref[...].T

    def body(i, _):
        base = i * 16
        for u in range(16):
            to_ref[pl.ds(idx_ref[base + u], 1), :] = rows_ref[pl.ds(base + u, 1), :]
        return 0

    lax.fori_loop(0, CH // 16, body, 0)

    @pl.when(pl.program_id(0) == pl.num_programs(0) - 1)
    def _():
        for s in range(0, o_ref.shape[1], CH):
            o_ref[:, s : s + CH] = to_ref[s : s + CH, :].T


def scatter_columns(idx, r):
    w, n = r.shape
    return pl.pallas_call(
        scatter_kernel,
        grid=(n // CH,),
        out_shape=jax.ShapeDtypeStruct((w, n), F32),
        in_specs=[
            pl.BlockSpec((CH,), lambda i: (i,), memory_space=pltpu.SMEM),
            pl.BlockSpec((w, CH), lambda i: (0, i)),
        ],
        out_specs=pl.BlockSpec((w, n), lambda i: (0, 0)),
        scratch_shapes=[pltpu.VMEM((CH, w), F32), pltpu.VMEM((n, w), F32)],
        compiler_params=pltpu.CompilerParams(vmem_limit_bytes=60 * 2**20),
        name="scatter",
    )(idx, r)


def exchange(slots, index, peers, ssem, rsem):
    here = slots.at[index]
    copies = [send(here, here, ssem.at[r], rsem.at[r], p) for r, p in enumerate(peers)]
    for c in copies:
        c.wait_recv()
    return copies


def tail_kernel(b_ref, t_ref, grp_ref, o_ref, res_ref, tot_ref,
                land_ref, want_ref, sq_ref, gr_ref, isem, tsem, osem, s2, r2, s3, r3):
    band, coef, _ = place()
    nband, bands, part = b_ref.shape
    ncoef = sq_ref.shape[0]
    bpeers = [(lax.rem(band + r, nband), coef) for r in range(1, nband)]
    cpeers = [(band, lax.rem(coef + r, ncoef)) for r in range(1, ncoef)]
    ins = []
    for s in range(nband):
        cols = pl.ds(s * part, part)
        ins.append(
            (
                pltpu.make_async_copy(b_ref.at[s], land_ref.at[:, cols], isem.at[s]),
                pltpu.make_async_copy(t_ref.at[:, cols], want_ref.at[:, cols], tsem.at[s]),
            )
        )
        for c in ins[-1]:
            c.start()
    barrier = pltpu.get_barrier_semaphore()
    for p in bpeers + cpeers:
        pl.semaphore_signal(barrier, inc=1, device_id=p, device_id_type=MESH)
    pl.semaphore_wait(barrier, nband + ncoef - 2)
    acc = jnp.zeros((bands, BLK), F32)
    outs = []
    for s in range(nband):
        for c in ins[s]:
            c.wait()
        cols = pl.ds(s * part, part)
        outs.append(pltpu.make_async_copy(land_ref.at[:, cols], o_ref.at[:, cols], osem.at[s]))
        outs[-1].start()
        d = land_ref[:, s * part : (s + 1) * part] - want_ref[:, s * part : (s + 1) * part]
        d = d * d
        for q in range(0, part, BLK):
            acc = acc + d[:, q : q + BLK]
    row = lax.broadcasted_iota(jnp.int32, (bands, BLK), 0)
    lane = lax.broadcasted_iota(jnp.int32, (bands, BLK), 1)
    total = jnp.sum(acc, axis=1, keepdims=True)
    line = jnp.sum(jnp.where(row == lane, total, 0.0), axis=0, keepdims=True)
    sq_ref[coef] = jnp.broadcast_to(line, (8, BLK))
    c2 = exchange(sq_ref, coef, cpeers, s2, r2)
    tot = sq_ref[0]
    for q in range(1, ncoef):
        tot = tot + sq_ref[q]
    res = jnp.sqrt(tot + 1e-06)
    res_ref[...] = res
    g16 = lax.broadcasted_iota(jnp.int32, (NGROUPS, BLK), 0)
    gr_ref[band] = jnp.where(g16 == grp_ref[0:1, :], res[0:1, :], 0.0)
    c3 = exchange(gr_ref, band, bpeers, s3, r3)
    g = gr_ref[0]
    for q in range(1, nband):
        g = g + gr_ref[q]
    tot_ref[...] = jnp.broadcast_to(jnp.sum(g, axis=1, keepdims=True), (NGROUPS, BLK)) * (NGROUPS / NB)
    for c in outs:
        c.wait()
    for c in c2 + c3:
        c.wait_send()


def tail(b, t, grp):
    vm = pl.BlockSpec(memory_space=pltpu.VMEM)
    bands, width = t.shape
    nband = b.shape[0]
    ncoef = lax.axis_size("coef")
    return pl.pallas_call(
        tail_kernel,
        out_shape=(
            jax.ShapeDtypeStruct((bands, width), F32),
            jax.ShapeDtypeStruct((8, BLK), F32),
            jax.ShapeDtypeStruct((NGROUPS, BLK), F32),
        ),
        in_specs=[ANY, ANY, vm],
        out_specs=(ANY, vm, vm),
        scratch_shapes=[
            pltpu.VMEM((bands, width), F32),
            pltpu.VMEM((bands, width), F32),
            pltpu.VMEM((ncoef, 8, BLK), F32),
            pltpu.VMEM((nband, NGROUPS, BLK), F32),
            pltpu.SemaphoreType.DMA((nband,)),
            pltpu.SemaphoreType.DMA((nband,)),
            pltpu.SemaphoreType.DMA((nband,)),
            pltpu.SemaphoreType.DMA((ncoef - 1,)),
            pltpu.SemaphoreType.DMA((ncoef - 1,)),
            pltpu.SemaphoreType.DMA((nband - 1,)),
            pltpu.SemaphoreType.DMA((nband - 1,)),
        ],
        compiler_params=pltpu.CompilerParams(
            collective_id=1, has_side_effects=True, vmem_limit_bytes=60 * 2**20
        ),
        name="tail",
    )(b, t, grp)


def local(coeffs, ref_block, index_map, band_group):
    bands, width = coeffs.shape
    parts = lax.axis_size("band")
    part = width // parts
    blocks = coeffs.reshape(bands, parts, part).transpose(1, 0, 2)
    columns = lax.all_to_all(blocks, "band", split_axis=0, concat_axis=0, tiled=True)
    columns = columns.reshape(parts * bands, part)
    moved = scatter_columns(index_map, ref_block)
    margin = reduce_all(gram(columns))
    ortho_cols = solve(margin, columns).reshape(parts, bands, part)
    back = lax.all_to_all(ortho_cols, "band", split_axis=0, concat_axis=0, tiled=True)
    groups = jnp.broadcast_to(jnp.pad(band_group, (0, BLK - bands), constant_values=-1), (8, BLK))
    ortho, res, tot = tail(back, moved, groups)
    return (ortho, res[0, :bands], tot[:, 0])


def solution(mesh):
    return jax.shard_map(
        local,
        mesh=mesh,
        in_specs=(P("band", "coef"), P("band", "coef"), P("coef"), P("band")),
        out_specs=(P("band", "coef"), P("band"), P()),
        check_vma=False,
    )
```

```python
import functools
import jax
import jax.numpy as jnp
from jax import lax
from jax.experimental import pallas as pl
from jax.experimental.pallas import tpu as pltpu
from jax.sharding import PartitionSpec as P

BLK = 128
PAN = 8
F32 = jnp.float32
BF = jnp.bfloat16


def split(x):
    hi = x.astype(BF)
    return hi, (x - hi.astype(F32)).astype(BF)


def dot3(ah, al, bh, bl, dims):
    d = functools.partial(lax.dot_general, dimension_numbers=(dims, ((), ())), preferred_element_type=F32)
    return d(ah, bh) + (d(ah, bl) + d(al, bh))


NN = ((1,), (0,))
NT = ((1,), (1,))


def lanes_of(x, lane):
    return jnp.take_along_axis(x, jnp.full(x.shape, lane, jnp.int32), axis=1)


def row_of(x, j):
    return jnp.broadcast_to(x[j : j + 1, :], (PAN, BLK))


def rows_sum(cols, rows):
    parts = [c * r for c, r in zip(cols, rows)]
    while len(parts) > 1:
        parts = [parts[i] + parts[i + 1] for i in range(0, len(parts), 2)]
    return parts[0]


def diag_inverse(a_ref, w_ref, m_ref):
    sub = lax.broadcasted_iota(jnp.int32, (PAN, BLK), 0)
    r_i = lax.broadcasted_iota(jnp.int32, (BLK, BLK), 0)
    c_i = lax.broadcasted_iota(jnp.int32, (BLK, BLK), 1)
    w_ref[...] = (r_i == c_i).astype(F32)

    def body(p, carry):
        x, *cols = carry
        base = pl.multiple_of(p * PAN, PAN)
        nxt = pl.multiple_of(jnp.minimum(base + PAN, BLK - PAN), PAN)
        fwd = w_ref[pl.ds(base, PAN), :]
        kw = fwd
        scale = jnp.zeros((PAN, BLK), F32)
        for j in range(PAN):
            d = row_of(cols[j], j)
            r = 1.0 / d
            f = cols[j] * r
            isj = sub == j
            for m in range(j + 1, PAN):
                b = row_of(cols[m], j)
                cols[m] = jnp.where(isj, b * r, cols[m] - f * b)
            b = row_of(x, j)
            x = jnp.where(isj, b * r, x - f * b)
            b = row_of(kw, j)
            kw = jnp.where(isj, b * r, kw - f * b)
            if j < PAN - 1:
                fwd = jnp.where(sub > j, fwd - f * row_of(fwd, j), fwd)
            scale = jnp.where(isj, lax.rsqrt(d), scale)
        m_ref[pl.ds(base, PAN), :] = fwd * scale
        xb = [row_of(x, m) for m in range(PAN)]
        kb = [row_of(kw, m) for m in range(PAN)]
        an = a_ref[pl.ds(nxt, PAN), :]
        xn = an - rows_sum([lanes_of(an, base + m) for m in range(PAN)], xb)
        new_cols = [lanes_of(xn, nxt + m) for m in range(PAN)]
        for s in range(0, BLK, PAN):
            a = a_ref[s : s + PAN, :]
            am = [lanes_of(a, base + m) for m in range(PAN)]
            a_ref[s : s + PAN, :] = a - rows_sum(am, xb)
            w_ref[s : s + PAN, :] = w_ref[s : s + PAN, :] - rows_sum(am, kb)
        return (xn, *new_cols)

    x0 = a_ref[0:PAN, :]
    lax.fori_loop(0, BLK // PAN, body, (x0, *[lanes_of(x0, m) for m in range(PAN)]))


MESH = pl.DeviceIdType.MESH
NB = 1024
NGROUPS = 16
NBLK = NB // BLK
TILES = NBLK * (NBLK + 1) // 2
ANY = pl.BlockSpec(memory_space=pltpu.HBM)


def tile_row(i, j):
    return (i * (i + 1) // 2 + j) * BLK


def place():
    band, coef = lax.axis_index("band"), lax.axis_index("coef")
    return band, coef, dict(z=band // 4, x=band % 4, y=coef // 2, core=coef % 2)


def peer_on(pos, dim, value):
    p = dict(pos)
    p[dim] = value
    return (p["z"] * 4 + p["x"], p["y"] * 2 + p["core"])


def send(src, dst, ssem, rsem, device):
    copy = pltpu.make_async_remote_copy(
        src_ref=src, dst_ref=dst, send_sem=ssem, recv_sem=rsem, device_id=device, device_id_type=MESH
    )
    copy.start()
    return copy


ORDERS = (("z", "x", "y"), ("x", "y", "z"), ("y", "z", "x"))
RING = 4
HALF = TILES * BLK // 2
PART = HALF // 3
Q1 = PART // RING
Q2 = Q1 // RING


def reduce_kernel(g_ref, o_ref, half_ref, b1_ref, a1_ref, b2_ref, b3_ref, csem, rsem, ssem):
    _, _, pos = place()
    partner = peer_on(pos, "core", 1 - pos["core"])
    peers = [partner] + [
        peer_on(pos, d, lax.rem(pos[d] + r, RING)) for d in ("z", "x", "y") for r in range(1, RING)
    ]
    barrier = pltpu.get_barrier_semaphore()
    for p in peers:
        pl.semaphore_signal(barrier, inc=1, device_id=p, device_id_type=MESH)
    pl.semaphore_wait(barrier, len(peers))

    core = pos["core"]
    mine = pl.multiple_of(core * HALF, PART)
    other = pl.multiple_of((1 - core) * HALF, PART)
    cs = [
        send(
            g_ref.at[pl.ds(pl.multiple_of(other + part * PART, PART), PART)],
            half_ref.at[part],
            csem.at[part],
            csem.at[3 + part],
            partner,
        )
        for part in range(3)
    ]
    c1 = []
    for part, (d1, _, _) in enumerate(ORDERS):
        cs[part].wait_recv()
        half_ref[part] = half_ref[part] + g_ref[pl.ds(pl.multiple_of(mine + part * PART, PART), PART), :]
        for r in (2, 1, 3):
            to = lax.rem(pos[d1] + r, RING)
            c1.append(
                send(
                    half_ref.at[part, pl.ds(pl.multiple_of(to * Q1, Q1), Q1)],
                    b1_ref.at[part, r - 1],
                    ssem.at[0, part, r - 1],
                    rsem.at[0, part, r - 1],
                    peer_on(pos, d1, to),
                )
            )
    c2 = []
    for part, (d1, d2, _) in enumerate(ORDERS):
        for c in c1[3 * part : 3 * part + 3]:
            c.wait_recv()
        own = half_ref[part, pl.ds(pl.multiple_of(pos[d1] * Q1, Q1), Q1), :]
        a1_ref[part] = own + b1_ref[part, 0] + (b1_ref[part, 1] + b1_ref[part, 2])
        for r in (2, 1, 3):
            to = lax.rem(pos[d2] + r, RING)
            c2.append(
                send(
                    a1_ref.at[part, pl.ds(pl.multiple_of(to * Q2, Q2), Q2)],
                    b2_ref.at[part, r - 1],
                    ssem.at[1, part, r - 1],
                    rsem.at[1, part, r - 1],
                    peer_on(pos, d2, to),
                )
            )
    c3 = []
    for part, (d1, d2, d3) in enumerate(ORDERS):
        for c in c2[3 * part : 3 * part + 3]:
            c.wait_recv()
        own = a1_ref[part, pl.ds(pl.multiple_of(pos[d2] * Q2, Q2), Q2), :]
        b3_ref[part, pos[d3]] = own + b2_ref[part, 0] + (b2_ref[part, 1] + b2_ref[part, 2])
        for r in (2, 1, 3):
            to = lax.rem(pos[d3] + r, RING)
            c3.append(
                send(
                    b3_ref.at[part, pos[d3]],
                    b3_ref.at[part, pos[d3]],
                    ssem.at[2, part, r - 1],
                    rsem.at[2, part, r - 1],
                    peer_on(pos, d3, to),
                )
            )
    c4 = []
    for part, (d1, d2, d3) in enumerate(ORDERS):
        for c in c3[3 * part : 3 * part + 3]:
            c.wait_recv()
        start = pl.multiple_of(mine + part * PART + pos[d1] * Q1 + pos[d2] * Q2, Q2)
        o_ref[pl.ds(start, Q2), :] = (b3_ref[part, 0] + b3_ref[part, 1]) + (b3_ref[part, 2] + b3_ref[part, 3])
        here = o_ref.at[pl.ds(start, Q2)]
        for r in (2, 1, 3):
            to = lax.rem(pos[d2] + r, RING)
            c4.append(send(here, here, ssem.at[3, part, r - 1], rsem.at[3, part, r - 1], peer_on(pos, d2, to)))
    c5 = []
    for part, (d1, d2, d3) in enumerate(ORDERS):
        for c in c4[3 * part : 3 * part + 3]:
            c.wait_recv()
        here = o_ref.at[pl.ds(pl.multiple_of(mine + part * PART + pos[d1] * Q1, Q2), Q1)]
        for r in (2, 1, 3):
            to = lax.rem(pos[d1] + r, RING)
            c5.append(send(here, here, ssem.at[4, part, r - 1], rsem.at[4, part, r - 1], peer_on(pos, d1, to)))
    c6 = []
    for part, (d1, d2, d3) in enumerate(ORDERS):
        for c in c5[3 * part : 3 * part + 3]:
            c.wait_recv()
        here = o_ref.at[pl.ds(pl.multiple_of(mine + part * PART, PART), PART)]
        c6.append(send(here, here, csem.at[6 + part], csem.at[9 + part], partner))
    for c in c6:
        c.wait_recv()
    for c in cs + c1 + c2 + c3 + c4 + c5 + c6:
        c.wait_send()


def reduce_all(g):
    return pl.pallas_call(
        reduce_kernel,
        out_shape=jax.ShapeDtypeStruct(g.shape, F32),
        in_specs=[pl.BlockSpec(memory_space=pltpu.VMEM)],
        out_specs=pl.BlockSpec(memory_space=pltpu.VMEM),
        scratch_shapes=[
            pltpu.VMEM((3, PART, BLK), F32),
            pltpu.VMEM((3, RING - 1, Q1, BLK), F32),
            pltpu.VMEM((3, Q1, BLK), F32),
            pltpu.VMEM((3, RING - 1, Q2, BLK), F32),
            pltpu.VMEM((3, RING, Q2, BLK), F32),
            pltpu.SemaphoreType.DMA((12,)),
            pltpu.SemaphoreType.DMA((5, 3, RING - 1)),
            pltpu.SemaphoreType.DMA((5, 3, RING - 1)),
        ],
        compiler_params=pltpu.CompilerParams(collective_id=0, has_side_effects=True, vmem_limit_bytes=60 * 2**20),
        name="reduce_all",
    )(g)


def solve_kernel(g_ref, c_ref, y_ref, a_ref, w_ref, m_ref, lh_ref, ll_ref, yh_ref, yl_ref, z_ref, csem, ysem):
    n = c_ref.shape[0]
    steps = n // BLK
    loads = []
    for k in range(steps):
        rows = pl.ds(k * BLK, BLK)
        loads.append(pltpu.make_async_copy(c_ref.at[rows], z_ref.at[rows], csem.at[k]))
        loads[-1].start()
    stores = []
    for k in range(steps):
        lo, hi = k * BLK, (k + 1) * BLK
        s = jnp.concatenate([g_ref[tile_row(i, k) : tile_row(i, k) + BLK, :] for i in range(k, steps)], axis=0)
        if k:
            s = s - dot3(lh_ref[lo:, :lo], ll_ref[lo:, :lo], lh_ref[lo:hi, :lo], ll_ref[lo:hi, :lo], NT)
        a_ref[...] = s[:BLK]
        diag_inverse(a_ref, w_ref, m_ref)
        mh, ml = split(m_ref[...])
        if hi < n:
            sh, sl = split(s[BLK:])
            lkh, lkl = split(dot3(sh, sl, mh, ml, NT))
            lh_ref[hi:, lo:hi] = lkh
            ll_ref[hi:, lo:hi] = lkl
        loads[k].wait()
        z = z_ref[lo:hi, :]
        if k:
            z = z - dot3(lh_ref[lo:hi, :lo], ll_ref[lo:hi, :lo], yh_ref[:lo, :], yl_ref[:lo, :], NN)
        zh, zl = split(z)
        y = dot3(mh, ml, zh, zl, NN)
        z_ref[lo:hi, :] = y
        rows = pl.ds(lo, BLK)
        stores.append(pltpu.make_async_copy(z_ref.at[rows], y_ref.at[rows], ysem.at[k]))
        stores[-1].start()
        if hi < n:
            yh, yl = split(y)
            yh_ref[lo:hi, :] = yh
            yl_ref[lo:hi, :] = yl
    for c in stores:
        c.wait()


def solve(g, c):
    n, w = c.shape
    return pl.pallas_call(
        solve_kernel,
        out_shape=jax.ShapeDtypeStruct((n, w), F32),
        in_specs=[pl.BlockSpec(memory_space=pltpu.VMEM), ANY],
        out_specs=ANY,
        scratch_shapes=[pltpu.VMEM((BLK, BLK), F32)] * 3
        + [pltpu.VMEM((n, n), BF)] * 2
        + [pltpu.VMEM((n, w), BF)] * 2
        + [pltpu.VMEM((n, w), F32), pltpu.SemaphoreType.DMA((n // BLK,)), pltpu.SemaphoreType.DMA((n // BLK,))],
        compiler_params=pltpu.CompilerParams(vmem_limit_bytes=60 * 2**20),
        name="solve",
    )(g, c)


GB = 256


def gram_kernel(c_ref, g_ref, x_ref, h_ref, l_ref, sem):
    n = c_ref.shape[0]
    loads = []
    for i in range(n // GB):
        rows = pl.ds(i * GB, GB)
        loads.append(pltpu.make_async_copy(c_ref.at[rows], x_ref.at[rows], sem.at[i]))
        loads[-1].start()
    for i in range(n // GB):
        lo, e = i * GB, (i + 1) * GB
        loads[i].wait()
        h, l = split(x_ref[lo:e, :])
        h_ref[lo:e, :] = h
        l_ref[lo:e, :] = l
        g = dot3(h, l, h_ref[:e, :], l_ref[:e, :], NT)
        for bi in range(lo // BLK, e // BLK):
            for bj in range(bi + 1):
                t = tile_row(bi, bj)
                r = bi * BLK - lo
                g_ref[t : t + BLK, :] = g[r : r + BLK, bj * BLK : (bj + 1) * BLK]


def gram(c):
    n, w = c.shape
    return pl.pallas_call(
        gram_kernel,
        out_shape=jax.ShapeDtypeStruct((TILES * BLK, BLK), F32),
        in_specs=[ANY],
        out_specs=pl.BlockSpec(memory_space=pltpu.VMEM),
        scratch_shapes=[
            pltpu.VMEM((n, w), F32),
            pltpu.VMEM((n, w), BF),
            pltpu.VMEM((n, w), BF),
            pltpu.SemaphoreType.DMA((n // GB,)),
        ],
        compiler_params=pltpu.CompilerParams(vmem_limit_bytes=60 * 2**20),
        name="gram",
    )(c)


HR = 32


def ring_kernel(to_rows, side, c_ref, o_ref, src_ref, land_ref, b1_ref, r1_ref, r2_ref,
                lsem, osem, s1, v1, sr1, vr1, sf1, s2, v2, sr2, vr2, sf2, qsem):
    band, coef, pos = place()
    part = 2048
    bands = 64
    dims = (("z", "x"), ("x", "z"))

    def who(h, a, b):
        d1, d2 = dims[h]
        p = dict(pos)
        p[d1] = lax.rem(pos[d1] + a + RING, RING)
        p[d2] = lax.rem(pos[d2] + b + RING, RING)
        return p["z"] * 4 + p["x"]

    def wide(h, b):
        return (pl.ds(h * HR, HR), pl.ds(pl.multiple_of(b * part, part), part))

    def tall(h, b):
        return (pl.ds(pl.multiple_of(b * bands + h * HR, HR), HR), slice(None))

    far = tall if to_rows else wide

    def cell(h, b):
        return (b, pl.ds(h * HR, HR))

    loads = {}
    for a in range(RING):
        for b in range(RING):
            d = who(0, a, b)
            at = (slice(None), pl.ds(pl.multiple_of(d * part, part), part)) if to_rows else (
                pl.ds(pl.multiple_of(d * bands, bands), bands), slice(None))
            loads[a, b] = pltpu.make_async_copy(c_ref.at[at], src_ref.at[d], lsem.at[a, b])
    order = [(2, 1), (1, 2), (2, 3), (3, 2), (2, 2), (2, 0), (0, 2)]
    order += [k for k in loads if k not in order and k != (0, 0)] + [(0, 0)]
    for k in order:
        loads[k].start()
    barrier = pltpu.get_barrier_semaphore()
    near_by = [(h, s) for h in range(2) for s in (1, -1)]
    for h, s in near_by:
        pl.semaphore_signal(barrier, inc=1, device_id=(who(h, s, 0), coef), device_id_type=MESH)
    pl.semaphore_wait(barrier, 4)

    ready = set()

    def src(h, a, b):
        k = (a, b) if h == 0 else (b, a)
        if k not in ready:
            loads[k].wait()
            ready.add(k)
        return src_ref.at[cell(h, who(h, a, b))]

    sent = []

    def go(*args):
        sent.append(send(*args))
        return sent[-1]

    SIGN = (1, -1)
    VIA1 = ((2, 1), (3, 0))
    VIA2 = ((0, 1), (3, 2))
    rel1 = {}
    for i in range(2):
        for h in range(2):
            for g in range(2):
                q = VIA1[g][i]
                rel1[h, g, i] = go(src(h, 2, q), r1_ref.at[h, g, i], sr1.at[h, g, i], vr1.at[h, g, i],
                                   (who(h, SIGN[g], 0), coef))
    dir1 = {}
    for q in (2, 1, 3, 0):
        for h in range(2):
            for g in range(2):
                r = 1 if g == 0 else 3
                dir1[h, r, q] = go(src(h, r, q), b1_ref.at[h, r - 1, q], s1.at[h, r - 1, q], v1.at[h, r - 1, q],
                                   (who(h, SIGN[g], 0), coef))
    side(0)
    for i in range(2):
        for h in range(2):
            for g in range(2):
                q = VIA1[g][i]
                rel1[h, g, i].wait_recv()
                dir1[h, 2, q] = go(r1_ref.at[h, g, i], b1_ref.at[h, 1, q], sf1.at[h, g, i], v1.at[h, 1, q],
                                   (who(h, SIGN[g], 0), coef))
    rel2, fin, outs = {}, {}, []

    def second(h, r, q):
        block = src(h, 0, q) if r == 0 else b1_ref.at[h, r - 1, q]
        if q == 0:
            at = far(h, who(h, -r, 0))
            outs.append(pltpu.make_async_copy(block, o_ref.at[at], qsem.at[h, r]))
            outs[-1].start()
        elif q == 2:
            g = 0 if r in VIA2[0] else 1
            i = VIA2[g].index(r)
            rel2[h, g, i] = go(block, r2_ref.at[h, g, i], sr2.at[h, g, i], vr2.at[h, g, i],
                               (who(h, 0, SIGN[g]), coef))
        else:
            at = land_ref.at[cell(h, who(h, -r, 0))]
            fin[h, r, q] = go(block, at, s2.at[h, r, q - 1], v2.at[h, r, q - 1],
                              (who(h, 0, 1 if q == 1 else -1), coef))

    for q in (2, 1, 3, 0):
        for h in range(2):
            second(h, 0, q)
    side(1)
    for q in (2, 1, 3, 0):
        for r in (1, 3):
            for h in range(2):
                dir1[h, r, q].wait_recv()
                second(h, r, q)
    for q in (2, 1, 3, 0):
        for h in range(2):
            dir1[h, 2, q].wait_recv()
            second(h, 2, q)
    side(2)
    for i in range(2):
        for h in range(2):
            for g in range(2):
                r = VIA2[g][i]
                rel2[h, g, i].wait_recv()
                at = land_ref.at[cell(h, who(h, -r, -SIGN[g]))]
                fin[h, r, 2] = go(r2_ref.at[h, g, i], at, sf2.at[h, g, i], v2.at[h, r, 1],
                                  (who(h, 0, SIGN[g]), coef))
    for r in (0, 1, 3, 2):
        for q in (1, 3, 2):
            for h in range(2):
                fin[h, r, q].wait_recv()
                b = who(h, -r, -q)
                outs.append(
                    pltpu.make_async_copy(land_ref.at[cell(h, b)], o_ref.at[far(h, b)], osem.at[h, r, q - 1])
                )
                outs[-1].start()
    for c in outs:
        c.wait()
    for c in sent:
        c.wait_send()


RING_SCRATCH = [
    pltpu.VMEM((16, 64, 2048), F32),
    pltpu.VMEM((16, 64, 2048), F32),
    pltpu.VMEM((2, 3, 4, HR, 2048), F32),
    pltpu.VMEM((2, 2, 2, HR, 2048), F32),
    pltpu.VMEM((2, 2, 2, HR, 2048), F32),
] + [
    pltpu.SemaphoreType.DMA(s)
    for s in (
        (4, 4), (2, 4, 3), (2, 3, 4), (2, 3, 4), (2, 2, 2), (2, 2, 2), (2, 2, 2),
        (2, 4, 3), (2, 4, 3), (2, 2, 2), (2, 2, 2), (2, 2, 2), (2, 4),
    )
]


def collect_kernel(c_ref, o_ref, *scratch):
    ring_kernel(False, lambda n: None, c_ref, o_ref, *scratch)


def collect(c):
    n, w = c.shape
    return pl.pallas_call(
        collect_kernel,
        out_shape=jax.ShapeDtypeStruct((n // 16, w * 16), F32),
        in_specs=[ANY],
        out_specs=ANY,
        scratch_shapes=RING_SCRATCH,
        compiler_params=pltpu.CompilerParams(
            collective_id=3, has_side_effects=True, vmem_limit_bytes=60 * 2**20
        ),
        name="collect",
    )(c)


CH = 2048
STOPS = (0, 12, 16)


def spread_kernel(inv_ref, c_ref, q_ref, o_ref, t_ref, q_all, rows_ref, got_ref, want_ref, isem, tsem, *scratch):
    bands, width = q_ref.shape
    n = width // CH
    loads = []
    for s in range(n):
        cols = pl.ds(s * CH, CH)
        loads.append(pltpu.make_async_copy(q_ref.at[:, cols], q_all.at[:, cols], isem.at[s]))
    stores = [
        pltpu.make_async_copy(want_ref.at[s % 2], t_ref.at[:, pl.ds(s * CH, CH)], tsem.at[s]) for s in range(n)
    ]

    def gather(s):
        def body(i, _):
            at = i * 16
            for u in range(16):
                got_ref[pl.ds(at + u, 1), :] = rows_ref[pl.ds(inv_ref[s * CH + at + u], 1), :]
            return 0

        lax.fori_loop(0, CH // 16, body, 0)
        if s >= 2:
            stores[s - 2].wait()
        want_ref[s % 2] = got_ref[...].T
        stores[s].start()

    def side(stage):
        if stage == 0:
            for c in loads:
                c.start()
            for s, c in enumerate(loads):
                c.wait()
                rows_ref[s * CH : (s + 1) * CH, :] = q_all[:, s * CH : (s + 1) * CH].T
        else:
            for s in range(STOPS[stage - 1], STOPS[stage]):
                gather(s)

    ring_kernel(True, side, c_ref, o_ref, *scratch)
    for c in stores[-2:]:
        c.wait()


def spread(inv, c, q):
    a, b = c.shape
    n = b // CH
    return pl.pallas_call(
        spread_kernel,
        out_shape=(jax.ShapeDtypeStruct((a * 16, b // 16), F32), jax.ShapeDtypeStruct(q.shape, F32)),
        in_specs=[pl.BlockSpec(memory_space=pltpu.SMEM), ANY, ANY],
        out_specs=(ANY, ANY),
        scratch_shapes=[
            pltpu.VMEM((a, b), F32),
            pltpu.VMEM((b, a), F32),
            pltpu.VMEM((CH, a), F32),
            pltpu.VMEM((2, a, CH), F32),
            pltpu.SemaphoreType.DMA((n,)),
            pltpu.SemaphoreType.DMA((n,)),
            *RING_SCRATCH,
        ],
        compiler_params=pltpu.CompilerParams(
            collective_id=2, has_side_effects=True, vmem_limit_bytes=60 * 2**20
        ),
        name="spread",
    )(inv, c, q)


def invert_kernel(idx_ref, inv_ref):
    n, w = idx_ref.shape
    his = n * w // BLK
    acc = jnp.zeros((his, 2 * BLK), F32)
    for c in range(n):
        idx = idx_ref[c : c + 1, :]
        at = c * w + lax.broadcasted_iota(jnp.int32, (1, w), 1)
        one = lax.broadcasted_iota(jnp.int32, (his, w), 0) == (idx >> 7)
        low = lax.broadcasted_iota(jnp.int32, (BLK, w), 0) == (idx & 127)
        hot = jnp.where(one, 1.0, 0.0).astype(BF)
        top = jnp.where(low, (at >> 7).astype(F32), 0.0).astype(BF)
        bot = jnp.where(low, (at & 127).astype(F32), 0.0).astype(BF)
        both = jnp.concatenate([top, bot], axis=0)
        acc = acc + lax.dot_general(hot, both, (NT, ((), ())), preferred_element_type=F32)
    inv_ref[...] = acc[:, :BLK].astype(jnp.int32) * BLK + acc[:, BLK:].astype(jnp.int32)


def invert(idx):
    n = idx.shape[0]
    out = pl.pallas_call(
        invert_kernel,
        out_shape=jax.ShapeDtypeStruct((n // BLK, BLK), jnp.int32),
        in_specs=[pl.BlockSpec(memory_space=pltpu.VMEM)],
        out_specs=pl.BlockSpec(memory_space=pltpu.VMEM),
        compiler_params=pltpu.CompilerParams(vmem_limit_bytes=60 * 2**20),
        name="invert",
    )(idx.reshape(16, n // 16))
    return out.reshape(n)


def exchange(slots, index, peers, ssem, rsem):
    here = slots.at[index]
    copies = [send(here, here, ssem.at[r], rsem.at[r], p) for r, p in enumerate(peers)]
    for c in copies:
        c.wait_recv()
    return copies


def tail_kernel(b_ref, t_ref, grp_ref, res_ref, tot_ref,
                land_ref, want_ref, sq_ref, gr_ref, isem, tsem, s2, r2, s3, r3):
    band, coef, _ = place()
    bands, width = b_ref.shape
    nband = gr_ref.shape[0]
    part = width // nband
    ncoef = sq_ref.shape[0]
    bpeers = [(lax.rem(band + r, nband), coef) for r in range(1, nband)]
    cpeers = [(band, lax.rem(coef + r, ncoef)) for r in range(1, ncoef)]
    ins = []
    for s in range(nband):
        cols = pl.ds(s * part, part)
        ins.append(
            (
                pltpu.make_async_copy(b_ref.at[:, cols], land_ref.at[:, cols], isem.at[s]),
                pltpu.make_async_copy(t_ref.at[:, cols], want_ref.at[:, cols], tsem.at[s]),
            )
        )
        for c in ins[-1]:
            c.start()
    barrier = pltpu.get_barrier_semaphore()
    for p in bpeers + cpeers:
        pl.semaphore_signal(barrier, inc=1, device_id=p, device_id_type=MESH)
    pl.semaphore_wait(barrier, nband + ncoef - 2)
    acc = jnp.zeros((bands, BLK), F32)
    for s in range(nband):
        for c in ins[s]:
            c.wait()
        d = land_ref[:, s * part : (s + 1) * part] - want_ref[:, s * part : (s + 1) * part]
        d = d * d
        for q in range(0, part, BLK):
            acc = acc + d[:, q : q + BLK]
    row = lax.broadcasted_iota(jnp.int32, (bands, BLK), 0)
    lane = lax.broadcasted_iota(jnp.int32, (bands, BLK), 1)
    total = jnp.sum(acc, axis=1, keepdims=True)
    line = jnp.sum(jnp.where(row == lane, total, 0.0), axis=0, keepdims=True)
    sq_ref[coef] = jnp.broadcast_to(line, (8, BLK))
    c2 = exchange(sq_ref, coef, cpeers, s2, r2)
    tot = sq_ref[0]
    for q in range(1, ncoef):
        tot = tot + sq_ref[q]
    res = jnp.sqrt(tot + 1e-06)
    res_ref[...] = res
    g16 = lax.broadcasted_iota(jnp.int32, (NGROUPS, BLK), 0)
    gr_ref[band] = jnp.where(g16 == grp_ref[0:1, :], res[0:1, :], 0.0)
    c3 = exchange(gr_ref, band, bpeers, s3, r3)
    g = gr_ref[0]
    for q in range(1, nband):
        g = g + gr_ref[q]
    tot_ref[...] = jnp.broadcast_to(jnp.sum(g, axis=1, keepdims=True), (NGROUPS, BLK)) * (NGROUPS / NB)
    for c in c2 + c3:
        c.wait_send()


def tail(b, t, grp):
    vm = pl.BlockSpec(memory_space=pltpu.VMEM)
    bands, width = t.shape
    nband = lax.axis_size("band")
    ncoef = lax.axis_size("coef")
    return pl.pallas_call(
        tail_kernel,
        out_shape=(
            jax.ShapeDtypeStruct((8, BLK), F32),
            jax.ShapeDtypeStruct((NGROUPS, BLK), F32),
        ),
        in_specs=[ANY, ANY, vm],
        out_specs=(vm, vm),
        scratch_shapes=[
            pltpu.VMEM((bands, width), F32),
            pltpu.VMEM((bands, width), F32),
            pltpu.VMEM((ncoef, 8, BLK), F32),
            pltpu.VMEM((nband, NGROUPS, BLK), F32),
            pltpu.SemaphoreType.DMA((nband,)),
            pltpu.SemaphoreType.DMA((nband,)),
            pltpu.SemaphoreType.DMA((ncoef - 1,)),
            pltpu.SemaphoreType.DMA((ncoef - 1,)),
            pltpu.SemaphoreType.DMA((nband - 1,)),
            pltpu.SemaphoreType.DMA((nband - 1,)),
        ],
        compiler_params=pltpu.CompilerParams(
            collective_id=1, has_side_effects=True, vmem_limit_bytes=60 * 2**20
        ),
        name="tail",
    )(b, t, grp)


def local(coeffs, ref_block, index_map, band_group):
    bands, _ = coeffs.shape
    columns, moved = spread(invert(index_map), coeffs, ref_block)
    margin = reduce_all(gram(columns))
    ortho = collect(solve(margin, columns))
    groups = jnp.broadcast_to(jnp.pad(band_group, (0, BLK - bands), constant_values=-1), (8, BLK))
    res, tot = tail(ortho, moved, groups)
    return (ortho, res[0, :bands], tot[:, 0])


def solution(mesh):
    return jax.shard_map(
        local,
        mesh=mesh,
        in_specs=(P("band", "coef"), P("band", "coef"), P("coef"), P("band")),
        out_specs=(P("band", "coef"), P("band"), P()),
        check_vma=False,
    )
```

```python
import functools
import jax
import jax.numpy as jnp
from jax import lax
from jax.experimental import pallas as pl
from jax.experimental.pallas import tpu as pltpu
from jax.sharding import PartitionSpec as P

BLK = 128
PAN = 16
F32 = jnp.float32
BF = jnp.bfloat16


def split(x):
    hi = x.astype(BF)
    return hi, (x - hi.astype(F32)).astype(BF)


def dot3(ah, al, bh, bl, dims):
    d = functools.partial(lax.dot_general, dimension_numbers=(dims, ((), ())), preferred_element_type=F32)
    return d(ah, bh) + (d(ah, bl) + d(al, bh))


NN = ((1,), (0,))
NT = ((1,), (1,))


def lanes_of(x, lane):
    return jnp.take_along_axis(x, jnp.full(x.shape, lane, jnp.int32), axis=1)


def row_of(x, j):
    return jnp.broadcast_to(x[j : j + 1, :], (PAN, BLK))


def rows_sum(cols, rows):
    parts = [c * r for c, r in zip(cols, rows)]
    while len(parts) > 1:
        parts = [parts[i] + parts[i + 1] for i in range(0, len(parts), 2)]
    return parts[0]


def diag_inverse(a_ref, w_ref, m_ref):
    sub = lax.broadcasted_iota(jnp.int32, (PAN, BLK), 0)
    r_i = lax.broadcasted_iota(jnp.int32, (BLK, BLK), 0)
    c_i = lax.broadcasted_iota(jnp.int32, (BLK, BLK), 1)
    w_ref[...] = (r_i == c_i).astype(F32)

    def body(p, carry):
        x, *cols = carry
        base = pl.multiple_of(p * PAN, PAN)
        nxt = pl.multiple_of(jnp.minimum(base + PAN, BLK - PAN), PAN)
        fwd = w_ref[pl.ds(base, PAN), :]
        kw = fwd
        scale = jnp.zeros((PAN, BLK), F32)
        for j in range(PAN):
            d = row_of(cols[j], j)
            r = 1.0 / d
            f = cols[j] * r
            isj = sub == j
            for m in range(j + 1, PAN):
                b = row_of(cols[m], j)
                cols[m] = jnp.where(isj, b * r, cols[m] - f * b)
            b = row_of(x, j)
            x = jnp.where(isj, b * r, x - f * b)
            b = row_of(kw, j)
            kw = jnp.where(isj, b * r, kw - f * b)
            if j < PAN - 1:
                fwd = jnp.where(sub > j, fwd - f * row_of(fwd, j), fwd)
            scale = jnp.where(isj, lax.rsqrt(d), scale)
        m_ref[pl.ds(base, PAN), :] = fwd * scale
        xb = [row_of(x, m) for m in range(PAN)]
        kb = [row_of(kw, m) for m in range(PAN)]
        an = a_ref[pl.ds(nxt, PAN), :]
        xn = an - rows_sum([lanes_of(an, base + m) for m in range(PAN)], xb)
        new_cols = [lanes_of(xn, nxt + m) for m in range(PAN)]
        raw = carry[0]
        rh, rm = split(raw)
        rl = (raw - rh.astype(F32) - rm.astype(F32)).astype(BF)
        bb = jnp.concatenate([x, kw], axis=1)
        bh, bm = split(bb)
        bl = (bb - bh.astype(F32) - bm.astype(F32)).astype(BF)
        f32 = lambda v: v.astype(F32)
        left = jnp.concatenate([f32(v) for v in (rh, rh, rm, rm, rh, rl)], axis=0).astype(BF)
        right = jnp.concatenate([f32(v) for v in (bh, bm, bh, bm, bl, bh)], axis=0).astype(BF)
        upd = lax.dot_general(left, right, (((0,), (0,)), ((), ())), preferred_element_type=F32)
        a_ref[...] = a_ref[...] - upd[:, :BLK]
        w_ref[...] = w_ref[...] - upd[:, BLK:]
        return (xn, *new_cols)

    x0 = a_ref[0:PAN, :]
    lax.fori_loop(0, BLK // PAN, body, (x0, *[lanes_of(x0, m) for m in range(PAN)]))


MESH = pl.DeviceIdType.MESH
NB = 1024
NGROUPS = 16
NBLK = NB // BLK
TILES = NBLK * (NBLK + 1) // 2
ANY = pl.BlockSpec(memory_space=pltpu.HBM)


def tile_row(i, j):
    return (i * (i + 1) // 2 + j) * BLK


def place():
    band, coef = lax.axis_index("band"), lax.axis_index("coef")
    return band, coef, dict(z=band // 4, x=band % 4, y=coef // 2, core=coef % 2)


def peer_on(pos, dim, value):
    p = dict(pos)
    p[dim] = value
    return (p["z"] * 4 + p["x"], p["y"] * 2 + p["core"])


def send(src, dst, ssem, rsem, device):
    copy = pltpu.make_async_remote_copy(
        src_ref=src, dst_ref=dst, send_sem=ssem, recv_sem=rsem, device_id=device, device_id_type=MESH
    )
    copy.start()
    return copy


ORDERS = (("z", "x", "y"), ("x", "y", "z"), ("y", "z", "x"))
RING = 4
HALF = TILES * BLK // 2
PART = HALF // 3
Q1 = PART // RING
Q2 = Q1 // RING


def reduce_kernel(g_ref, o_ref, half_ref, b1_ref, a1_ref, b2_ref, b3_ref, csem, rsem, ssem):
    _, _, pos = place()
    partner = peer_on(pos, "core", 1 - pos["core"])
    peers = [partner] + [
        peer_on(pos, d, lax.rem(pos[d] + r, RING)) for d in ("z", "x", "y") for r in range(1, RING)
    ]
    barrier = pltpu.get_barrier_semaphore()
    for p in peers:
        pl.semaphore_signal(barrier, inc=1, device_id=p, device_id_type=MESH)
    pl.semaphore_wait(barrier, len(peers))

    core = pos["core"]
    mine = pl.multiple_of(core * HALF, PART)
    other = pl.multiple_of((1 - core) * HALF, PART)
    cs = [
        send(
            g_ref.at[pl.ds(pl.multiple_of(other + part * PART, PART), PART)],
            half_ref.at[part],
            csem.at[part],
            csem.at[3 + part],
            partner,
        )
        for part in range(3)
    ]
    c1 = []
    for part, (d1, _, _) in enumerate(ORDERS):
        cs[part].wait_recv()
        half_ref[part] = half_ref[part] + g_ref[pl.ds(pl.multiple_of(mine + part * PART, PART), PART), :]
        for r in (2, 1, 3):
            to = lax.rem(pos[d1] + r, RING)
            c1.append(
                send(
                    half_ref.at[part, pl.ds(pl.multiple_of(to * Q1, Q1), Q1)],
                    b1_ref.at[part, r - 1],
                    ssem.at[0, part, r - 1],
                    rsem.at[0, part, r - 1],
                    peer_on(pos, d1, to),
                )
            )
    c2 = []
    for part, (d1, d2, _) in enumerate(ORDERS):
        for c in c1[3 * part : 3 * part + 3]:
            c.wait_recv()
        own = half_ref[part, pl.ds(pl.multiple_of(pos[d1] * Q1, Q1), Q1), :]
        a1_ref[part] = own + b1_ref[part, 0] + (b1_ref[part, 1] + b1_ref[part, 2])
        for r in (2, 1, 3):
            to = lax.rem(pos[d2] + r, RING)
            c2.append(
                send(
                    a1_ref.at[part, pl.ds(pl.multiple_of(to * Q2, Q2), Q2)],
                    b2_ref.at[part, r - 1],
                    ssem.at[1, part, r - 1],
                    rsem.at[1, part, r - 1],
                    peer_on(pos, d2, to),
                )
            )
    c3 = []
    for part, (d1, d2, d3) in enumerate(ORDERS):
        for c in c2[3 * part : 3 * part + 3]:
            c.wait_recv()
        own = a1_ref[part, pl.ds(pl.multiple_of(pos[d2] * Q2, Q2), Q2), :]
        b3_ref[part, pos[d3]] = own + b2_ref[part, 0] + (b2_ref[part, 1] + b2_ref[part, 2])
        for r in (2, 1, 3):
            to = lax.rem(pos[d3] + r, RING)
            c3.append(
                send(
                    b3_ref.at[part, pos[d3]],
                    b3_ref.at[part, pos[d3]],
                    ssem.at[2, part, r - 1],
                    rsem.at[2, part, r - 1],
                    peer_on(pos, d3, to),
                )
            )
    c4 = []
    for part, (d1, d2, d3) in enumerate(ORDERS):
        for c in c3[3 * part : 3 * part + 3]:
            c.wait_recv()
        start = pl.multiple_of(mine + part * PART + pos[d1] * Q1 + pos[d2] * Q2, Q2)
        o_ref[pl.ds(start, Q2), :] = (b3_ref[part, 0] + b3_ref[part, 1]) + (b3_ref[part, 2] + b3_ref[part, 3])
        here = o_ref.at[pl.ds(start, Q2)]
        for r in (2, 1, 3):
            to = lax.rem(pos[d2] + r, RING)
            c4.append(send(here, here, ssem.at[3, part, r - 1], rsem.at[3, part, r - 1], peer_on(pos, d2, to)))
    c5 = []
    for part, (d1, d2, d3) in enumerate(ORDERS):
        for c in c4[3 * part : 3 * part + 3]:
            c.wait_recv()
        here = o_ref.at[pl.ds(pl.multiple_of(mine + part * PART + pos[d1] * Q1, Q2), Q1)]
        for r in (2, 1, 3):
            to = lax.rem(pos[d1] + r, RING)
            c5.append(send(here, here, ssem.at[4, part, r - 1], rsem.at[4, part, r - 1], peer_on(pos, d1, to)))
    c6 = []
    for part, (d1, d2, d3) in enumerate(ORDERS):
        for c in c5[3 * part : 3 * part + 3]:
            c.wait_recv()
        here = o_ref.at[pl.ds(pl.multiple_of(mine + part * PART, PART), PART)]
        c6.append(send(here, here, csem.at[6 + part], csem.at[9 + part], partner))
    for c in c6:
        c.wait_recv()
    for c in cs + c1 + c2 + c3 + c4 + c5 + c6:
        c.wait_send()


def reduce_all(g):
    return pl.pallas_call(
        reduce_kernel,
        out_shape=jax.ShapeDtypeStruct(g.shape, F32),
        in_specs=[pl.BlockSpec(memory_space=pltpu.VMEM)],
        out_specs=pl.BlockSpec(memory_space=pltpu.VMEM),
        scratch_shapes=[
            pltpu.VMEM((3, PART, BLK), F32),
            pltpu.VMEM((3, RING - 1, Q1, BLK), F32),
            pltpu.VMEM((3, Q1, BLK), F32),
            pltpu.VMEM((3, RING - 1, Q2, BLK), F32),
            pltpu.VMEM((3, RING, Q2, BLK), F32),
            pltpu.SemaphoreType.DMA((12,)),
            pltpu.SemaphoreType.DMA((5, 3, RING - 1)),
            pltpu.SemaphoreType.DMA((5, 3, RING - 1)),
        ],
        compiler_params=pltpu.CompilerParams(collective_id=0, has_side_effects=True, vmem_limit_bytes=60 * 2**20),
        name="reduce_all",
    )(g)


def solve_kernel(g_ref, c_ref, y_ref, a_ref, w_ref, m_ref, lh_ref, ll_ref, yh_ref, yl_ref, z_ref, csem, ysem):
    n = c_ref.shape[0]
    steps = n // BLK
    loads = []
    for k in range(steps):
        rows = pl.ds(k * BLK, BLK)
        loads.append(pltpu.make_async_copy(c_ref.at[rows], z_ref.at[rows], csem.at[k]))
        loads[-1].start()
    stores = []
    for k in range(steps):
        lo, hi = k * BLK, (k + 1) * BLK
        s = jnp.concatenate([g_ref[tile_row(i, k) : tile_row(i, k) + BLK, :] for i in range(k, steps)], axis=0)
        if k:
            s = s - dot3(lh_ref[lo:, :lo], ll_ref[lo:, :lo], lh_ref[lo:hi, :lo], ll_ref[lo:hi, :lo], NT)
        a_ref[...] = s[:BLK]
        diag_inverse(a_ref, w_ref, m_ref)
        mh, ml = split(m_ref[...])
        if hi < n:
            sh, sl = split(s[BLK:])
            lkh, lkl = split(dot3(sh, sl, mh, ml, NT))
            lh_ref[hi:, lo:hi] = lkh
            ll_ref[hi:, lo:hi] = lkl
        loads[k].wait()
        z = z_ref[lo:hi, :]
        if k:
            z = z - dot3(lh_ref[lo:hi, :lo], ll_ref[lo:hi, :lo], yh_ref[:lo, :], yl_ref[:lo, :], NN)
        zh, zl = split(z)
        y = dot3(mh, ml, zh, zl, NN)
        z_ref[lo:hi, :] = y
        rows = pl.ds(lo, BLK)
        stores.append(pltpu.make_async_copy(z_ref.at[rows], y_ref.at[rows], ysem.at[k]))
        stores[-1].start()
        if hi < n:
            yh, yl = split(y)
            yh_ref[lo:hi, :] = yh
            yl_ref[lo:hi, :] = yl
    for c in stores:
        c.wait()


def solve(g, c):
    n, w = c.shape
    return pl.pallas_call(
        solve_kernel,
        out_shape=jax.ShapeDtypeStruct((n, w), F32),
        in_specs=[pl.BlockSpec(memory_space=pltpu.VMEM), ANY],
        out_specs=ANY,
        scratch_shapes=[pltpu.VMEM((BLK, BLK), F32)] * 3
        + [pltpu.VMEM((n, n), BF)] * 2
        + [pltpu.VMEM((n, w), BF)] * 2
        + [pltpu.VMEM((n, w), F32), pltpu.SemaphoreType.DMA((n // BLK,)), pltpu.SemaphoreType.DMA((n // BLK,))],
        compiler_params=pltpu.CompilerParams(vmem_limit_bytes=60 * 2**20),
        name="solve",
    )(g, c)


GB = 256


def gram_kernel(c_ref, g_ref, x_ref, h_ref, l_ref, sem):
    n = c_ref.shape[0]
    loads = []
    for i in range(n // GB):
        rows = pl.ds(i * GB, GB)
        loads.append(pltpu.make_async_copy(c_ref.at[rows], x_ref.at[rows], sem.at[i]))
        loads[-1].start()
    for i in range(n // GB):
        lo, e = i * GB, (i + 1) * GB
        loads[i].wait()
        h, l = split(x_ref[lo:e, :])
        h_ref[lo:e, :] = h
        l_ref[lo:e, :] = l
        g = dot3(h, l, h_ref[:e, :], l_ref[:e, :], NT)
        for bi in range(lo // BLK, e // BLK):
            for bj in range(bi + 1):
                t = tile_row(bi, bj)
                r = bi * BLK - lo
                g_ref[t : t + BLK, :] = g[r : r + BLK, bj * BLK : (bj + 1) * BLK]


def gram(c):
    n, w = c.shape
    return pl.pallas_call(
        gram_kernel,
        out_shape=jax.ShapeDtypeStruct((TILES * BLK, BLK), F32),
        in_specs=[ANY],
        out_specs=pl.BlockSpec(memory_space=pltpu.VMEM),
        scratch_shapes=[
            pltpu.VMEM((n, w), F32),
            pltpu.VMEM((n, w), BF),
            pltpu.VMEM((n, w), BF),
            pltpu.SemaphoreType.DMA((n // GB,)),
        ],
        compiler_params=pltpu.CompilerParams(vmem_limit_bytes=60 * 2**20),
        name="gram",
    )(c)


HR = 32


def ring_kernel(to_rows, greet, side, done, c_ref, o_ref, src_ref, land_ref, b1_ref, r1_ref, r2_ref,
                lsem, osem, s1, v1, sr1, vr1, sf1, s2, v2, sr2, vr2, sf2, qsem):
    band, coef, pos = place()
    part = 2048
    bands = 64
    dims = (("z", "x"), ("x", "z"))

    def who(h, a, b):
        d1, d2 = dims[h]
        p = dict(pos)
        p[d1] = lax.rem(pos[d1] + a + RING, RING)
        p[d2] = lax.rem(pos[d2] + b + RING, RING)
        return p["z"] * 4 + p["x"]

    def wide(h, b):
        return (pl.ds(h * HR, HR), pl.ds(pl.multiple_of(b * part, part), part))

    def tall(h, b):
        return (pl.ds(pl.multiple_of(b * bands + h * HR, HR), HR), slice(None))

    far = tall if to_rows else wide

    def cell(h, b):
        return (b, pl.ds(h * HR, HR))

    loads = {}
    for a in range(RING):
        for b in range(RING):
            d = who(0, a, b)
            at = (slice(None), pl.ds(pl.multiple_of(d * part, part), part)) if to_rows else (
                pl.ds(pl.multiple_of(d * bands, bands), bands), slice(None))
            loads[a, b] = pltpu.make_async_copy(c_ref.at[at], src_ref.at[d], lsem.at[a, b])
    order = [(2, 1), (1, 2), (2, 3), (3, 2), (2, 2), (2, 0), (0, 2)]
    order += [k for k in loads if k not in order and k != (0, 0)] + [(0, 0)]
    for k in order:
        loads[k].start()
    peers = greet(band, coef) if greet else [
        (who(h, s, 0), coef) for h in range(2) for s in (1, -1)
    ]
    barrier = pltpu.get_barrier_semaphore()
    for p in peers:
        pl.semaphore_signal(barrier, inc=1, device_id=p, device_id_type=MESH)
    pl.semaphore_wait(barrier, len(peers))

    ready = set()

    def src(h, a, b):
        k = (a, b) if h == 0 else (b, a)
        if k not in ready:
            loads[k].wait()
            ready.add(k)
        return src_ref.at[cell(h, who(h, a, b))]

    sent = []

    def go(*args):
        sent.append(send(*args))
        return sent[-1]

    SIGN = (1, -1)
    VIA1 = ((2, 1), (3, 0))
    VIA2 = ((0, 1), (3, 2))
    rel1 = {}
    for i in range(2):
        for h in range(2):
            for g in range(2):
                q = VIA1[g][i]
                rel1[h, g, i] = go(src(h, 2, q), r1_ref.at[h, g, i], sr1.at[h, g, i], vr1.at[h, g, i],
                                   (who(h, SIGN[g], 0), coef))
    dir1 = {}
    for q in (2, 1, 3, 0):
        for h in range(2):
            for g in range(2):
                r = 1 if g == 0 else 3
                dir1[h, r, q] = go(src(h, r, q), b1_ref.at[h, r - 1, q], s1.at[h, r - 1, q], v1.at[h, r - 1, q],
                                   (who(h, SIGN[g], 0), coef))
    side(0)
    for i in range(2):
        for h in range(2):
            for g in range(2):
                q = VIA1[g][i]
                rel1[h, g, i].wait_recv()
                dir1[h, 2, q] = go(r1_ref.at[h, g, i], b1_ref.at[h, 1, q], sf1.at[h, g, i], v1.at[h, 1, q],
                                   (who(h, SIGN[g], 0), coef))
    rel2, fin, outs = {}, {}, []

    def second(h, r, q):
        block = src(h, 0, q) if r == 0 else b1_ref.at[h, r - 1, q]
        if q == 0:
            at = far(h, who(h, -r, 0))
            outs.append(pltpu.make_async_copy(block, o_ref.at[at], qsem.at[h, r]))
            outs[-1].start()
        elif q == 2:
            g = 0 if r in VIA2[0] else 1
            i = VIA2[g].index(r)
            rel2[h, g, i] = go(block, r2_ref.at[h, g, i], sr2.at[h, g, i], vr2.at[h, g, i],
                               (who(h, 0, SIGN[g]), coef))
        else:
            at = land_ref.at[cell(h, who(h, -r, 0))]
            fin[h, r, q] = go(block, at, s2.at[h, r, q - 1], v2.at[h, r, q - 1],
                              (who(h, 0, 1 if q == 1 else -1), coef))

    for q in (2, 1, 3, 0):
        for h in range(2):
            second(h, 0, q)
    side(1)
    for q in (2, 1, 3, 0):
        for r in (1, 3):
            for h in range(2):
                dir1[h, r, q].wait_recv()
                second(h, r, q)
        side(2)
    for n, q in enumerate((2, 3, 1, 0)):
        for h in range(2):
            dir1[h, 2, q].wait_recv()
            second(h, 2, q)
        if n % 2:
            side(3)
    for i in range(2):
        for h in range(2):
            for g in range(2):
                r = VIA2[g][i]
                rel2[h, g, i].wait_recv()
                at = land_ref.at[cell(h, who(h, -r, -SIGN[g]))]
                fin[h, r, 2] = go(r2_ref.at[h, g, i], at, sf2.at[h, g, i], v2.at[h, r, 1],
                                  (who(h, 0, SIGN[g]), coef))
    side(4)
    for r in range(RING):
        for h in range(2):
            b = who(h, -r, 0)
            done(h, b, src_ref.at[cell(h, band)] if r == 0 else b1_ref.at[h, r - 1, 0])
    for r in (0, 1, 3, 2):
        for q in (1, 3, 2):
            for h in range(2):
                fin[h, r, q].wait_recv()
                b = who(h, -r, -q)
                done(h, b, land_ref.at[cell(h, b)])
                outs.append(
                    pltpu.make_async_copy(land_ref.at[cell(h, b)], o_ref.at[far(h, b)], osem.at[h, r, q - 1])
                )
                outs[-1].start()
    for c in sent:
        c.wait_send()
    return outs


RING_SCRATCH = [
    pltpu.VMEM((16, 64, 2048), F32),
    pltpu.VMEM((16, 64, 2048), F32),
    pltpu.VMEM((2, 3, 4, HR, 2048), F32),
    pltpu.VMEM((2, 2, 2, HR, 2048), F32),
    pltpu.VMEM((2, 2, 2, HR, 2048), F32),
] + [
    pltpu.SemaphoreType.DMA(s)
    for s in (
        (4, 4), (2, 4, 3), (2, 3, 4), (2, 3, 4), (2, 2, 2), (2, 2, 2), (2, 2, 2),
        (2, 4, 3), (2, 4, 3), (2, 2, 2), (2, 2, 2), (2, 2, 2), (2, 4),
    )
]


def exchange(slots, index, peers, ssem, rsem):
    here = slots.at[index]
    copies = [send(here, here, ssem.at[r], rsem.at[r], p) for r, p in enumerate(peers)]
    for c in copies:
        c.wait_recv()
    return copies


CH = 2048


def spread_kernel(idx_ref, c_ref, o_ref, inv_ref, acc_ref, *scratch):
    tall_, lanes_ = idx_ref.shape
    group = 16

    def side(stage):
        if stage:
            return
        acc_ref[...] = jnp.zeros_like(acc_ref)
        lane = lax.broadcasted_iota(jnp.int32, (BLK, lanes_), 1)
        his = lax.broadcasted_iota(jnp.int32, (tall_, lanes_), 0)
        los = lax.broadcasted_iota(jnp.int32, (BLK, lanes_), 0)

        def body(c, _):
            hots, boths = [], []
            for u in range(group):
                row = c * group + u
                idx = idx_ref[pl.ds(row, 1), :]
                hots.append(jnp.where(his == (idx >> 7), 1.0, 0.0).astype(BF))
                low = los == (idx & 127)
                top = jnp.where(low, jnp.full((BLK, lanes_), row, jnp.int32).astype(F32), 0.0)
                bot = jnp.where(low, lane.astype(F32), 0.0)
                boths.append(jnp.concatenate([top, bot], axis=0).astype(BF))
            acc_ref[...] += lax.dot_general(
                jnp.concatenate(hots, axis=1),
                jnp.concatenate(boths, axis=1),
                (NT, ((), ())),
                preferred_element_type=F32,
            )
            return 0

        lax.fori_loop(0, tall_ // group, body, 0)
        inv_ref[...] = acc_ref[:, :BLK].astype(jnp.int32) * BLK + acc_ref[:, BLK:].astype(jnp.int32)

    outs = ring_kernel(True, None, side, lambda *a: None, c_ref, o_ref, *scratch)
    for c in outs:
        c.wait()


def spread(idx, c):
    a, b = c.shape
    vm = pl.BlockSpec(memory_space=pltpu.VMEM)
    return pl.pallas_call(
        spread_kernel,
        out_shape=(
            jax.ShapeDtypeStruct((a * 16, b // 16), F32),
            jax.ShapeDtypeStruct((b // BLK, BLK), jnp.int32),
        ),
        in_specs=[vm, ANY],
        out_specs=(ANY, vm),
        scratch_shapes=[pltpu.VMEM((b // BLK, 2 * BLK), F32), *RING_SCRATCH],
        compiler_params=pltpu.CompilerParams(
            collective_id=2, has_side_effects=True, vmem_limit_bytes=60 * 2**20
        ),
        name="spread",
    )(idx.reshape(b // BLK, BLK), c)


STOPS = (0, 2, 4, 6, 8, 10, 12, 14, 16)


def collect_kernel(inv_ref, y_ref, q_ref, grp_ref, o_ref, res_ref, tot_ref,
                   want_ref, rows_ref, got_ref, acc_ref, sq_ref, gr_ref, isem, s2, r2, s3, r3, *scratch):
    band, coef, _ = place()
    nband, ncoef = gr_ref.shape[0], sq_ref.shape[0]
    bands, width = q_ref.shape
    n = width // CH
    bpeers = [(lax.rem(band + r, nband), coef) for r in range(1, nband)]
    cpeers = [(band, lax.rem(coef + r, ncoef)) for r in range(1, ncoef)]

    def columns(s):
        return pl.ds(pl.multiple_of(s * CH, CH), CH)

    def load(s):
        return pltpu.make_async_copy(q_ref.at[:, columns(s)], want_ref.at[:, columns(s)], isem.at[s])

    def turn(s, _):
        load(s).wait()
        rows_ref[columns(s), :] = want_ref[:, columns(s)].T
        return 0

    def gather(s, _):
        def body(i, _):
            at = i * 16
            for u in range(16):
                got_ref[pl.ds(at + u, 1), :] = rows_ref[pl.ds(inv_ref[s * CH + at + u], 1), :]
            return 0

        lax.fori_loop(0, CH // 16, body, 0)
        want_ref[:, columns(s)] = got_ref[...].T
        return 0

    calls = []

    def side(stage):
        if stage == 0:
            acc_ref[...] = jnp.zeros_like(acc_ref)
            for s in range(n):
                load(s).start()
            lax.fori_loop(0, n, turn, 0)
            return
        k = len(calls)
        calls.append(stage)
        last = STOPS[k + 1] if stage < 4 else n
        lax.fori_loop(STOPS[k], last, gather, 0)

    def done(h, b, block):
        step = 4 * BLK

        def body(i, acc):
            at = pl.multiple_of(i * step, step)
            d = block[:, pl.ds(at, step)] - want_ref[pl.ds(h * HR, HR), pl.ds(pl.multiple_of(b * CH + at, step), step)]
            d = d * d
            return acc + ((d[:, :BLK] + d[:, BLK : 2 * BLK]) + (d[:, 2 * BLK : 3 * BLK] + d[:, 3 * BLK :]))

        acc_ref[h] = lax.fori_loop(0, CH // step, body, acc_ref[h])

    outs = ring_kernel(False, lambda *a: bpeers + cpeers, side, done, y_ref, o_ref, *scratch)

    row = lax.broadcasted_iota(jnp.int32, (bands, BLK), 0)
    lane = lax.broadcasted_iota(jnp.int32, (bands, BLK), 1)
    total = jnp.sum(jnp.concatenate([acc_ref[0], acc_ref[1]], axis=0), axis=1, keepdims=True)
    line = jnp.sum(jnp.where(row == lane, total, 0.0), axis=0, keepdims=True)
    sq_ref[coef] = jnp.broadcast_to(line, (8, BLK))
    c2 = exchange(sq_ref, coef, cpeers, s2, r2)
    tot = sq_ref[0]
    for q in range(1, ncoef):
        tot = tot + sq_ref[q]
    res = jnp.sqrt(tot + 1e-06)
    res_ref[...] = res
    g16 = lax.broadcasted_iota(jnp.int32, (NGROUPS, BLK), 0)
    gr_ref[band] = jnp.where(g16 == grp_ref[0:1, :], res[0:1, :], 0.0)
    c3 = exchange(gr_ref, band, bpeers, s3, r3)
    g = gr_ref[0]
    for q in range(1, nband):
        g = g + gr_ref[q]
    row = lax.broadcasted_iota(jnp.int32, (NGROUPS, BLK), 0)
    lane = lax.broadcasted_iota(jnp.int32, (NGROUPS, BLK), 1)
    g = jnp.sum(g, axis=1, keepdims=True) * (NGROUPS / NB)
    tot_ref[...] = jnp.broadcast_to(jnp.sum(jnp.where(row == lane, g, 0.0), axis=0, keepdims=True), (8, BLK))
    for c in outs:
        c.wait()
    for c in c2 + c3:
        c.wait_send()


def collect(inv, y, q, grp):
    bands, width = q.shape
    vm = pl.BlockSpec(memory_space=pltpu.VMEM)
    nband, ncoef = lax.axis_size("band"), lax.axis_size("coef")
    dma = pltpu.SemaphoreType.DMA
    return pl.pallas_call(
        collect_kernel,
        out_shape=(
            jax.ShapeDtypeStruct((bands, width), F32),
            jax.ShapeDtypeStruct((8, BLK), F32),
            jax.ShapeDtypeStruct((8, BLK), F32),
        ),
        in_specs=[pl.BlockSpec(memory_space=pltpu.SMEM), ANY, ANY, vm],
        out_specs=(ANY, vm, vm),
        scratch_shapes=[
            pltpu.VMEM((bands, width), F32),
            pltpu.VMEM((width, bands), F32),
            pltpu.VMEM((CH, bands), F32),
            pltpu.VMEM((2, HR, BLK), F32),
            pltpu.VMEM((ncoef, 8, BLK), F32),
            pltpu.VMEM((nband, NGROUPS, BLK), F32),
            dma((width // CH,)),
            dma((ncoef - 1,)),
            dma((ncoef - 1,)),
            dma((nband - 1,)),
            dma((nband - 1,)),
            *RING_SCRATCH,
        ],
        compiler_params=pltpu.CompilerParams(
            collective_id=3, has_side_effects=True, vmem_limit_bytes=60 * 2**20
        ),
        name="collect",
    )(inv.reshape(width), y, q, grp)


def finish_kernel(raw_ref, res_ref, tot_ref, o_ref, band_ref, group_ref, buf_ref, isem, osem):
    n = raw_ref.shape[0] // 8
    ins = [pltpu.make_async_copy(raw_ref.at[pl.ds(8 * s, 8)], buf_ref.at[s], isem.at[s]) for s in range(n)]
    outs = [pltpu.make_async_copy(buf_ref.at[s], o_ref.at[pl.ds(8 * s, 8)], osem.at[s]) for s in range(n)]
    for c in ins:
        c.start()
    band_ref[...] = res_ref[0, : band_ref.shape[0]]
    group_ref[...] = tot_ref[0, : group_ref.shape[0]]
    for a, b in zip(ins, outs):
        a.wait()
        b.start()
    for c in outs:
        c.wait()


def finish(raw, res, tot):
    bands, width = raw.shape
    vm = pl.BlockSpec(memory_space=pltpu.VMEM)
    return pl.pallas_call(
        finish_kernel,
        out_shape=(
            jax.ShapeDtypeStruct((bands, width), F32),
            jax.ShapeDtypeStruct((bands,), F32),
            jax.ShapeDtypeStruct((NGROUPS,), F32),
        ),
        in_specs=[ANY, vm, vm],
        out_specs=(ANY, vm, vm),
        scratch_shapes=[
            pltpu.VMEM((bands // 8, 8, width), F32),
            pltpu.SemaphoreType.DMA((bands // 8,)),
            pltpu.SemaphoreType.DMA((bands // 8,)),
        ],
        compiler_params=pltpu.CompilerParams(vmem_limit_bytes=60 * 2**20),
        name="finish",
    )(raw, res, tot)


def local(coeffs, ref_block, index_map, band_group):
    bands, _ = coeffs.shape
    columns, inv = spread(index_map, coeffs)
    margin = reduce_all(gram(columns))
    groups = jnp.broadcast_to(jnp.pad(band_group, (0, BLK - bands), constant_values=-1), (8, BLK))
    return finish(*collect(inv, solve(margin, columns), ref_block, groups))


def solution(mesh):
    return jax.shard_map(
        local,
        mesh=mesh,
        in_specs=(P("band", "coef"), P("band", "coef"), P("coef"), P("band")),
        out_specs=(P("band", "coef"), P("band"), P()),
        check_vma=False,
    )
```

```python
import functools
import jax
import jax.numpy as jnp
from jax import lax
from jax.experimental import pallas as pl
from jax.experimental.pallas import tpu as pltpu
from jax.sharding import PartitionSpec as P

BLK = 128
PAN = 16
F32 = jnp.float32
BF = jnp.bfloat16


def split(x):
    hi = x.astype(BF)
    return hi, (x - hi.astype(F32)).astype(BF)


def dot3(ah, al, bh, bl, dims):
    d = functools.partial(lax.dot_general, dimension_numbers=(dims, ((), ())), preferred_element_type=F32)
    return d(ah, bh) + (d(ah, bl) + d(al, bh))


NN = ((1,), (0,))
NT = ((1,), (1,))


def lanes_of(x, lane):
    return jnp.take_along_axis(x, jnp.full(x.shape, lane, jnp.int32), axis=1)


def row_of(x, j):
    return jnp.broadcast_to(x[j : j + 1, :], (PAN, BLK))


def rows_sum(cols, rows):
    parts = [c * r for c, r in zip(cols, rows)]
    while len(parts) > 1:
        parts = [parts[i] + parts[i + 1] for i in range(0, len(parts), 2)]
    return parts[0]


def diag_inverse(a_ref, w_ref, m_ref, side):
    sub = lax.broadcasted_iota(jnp.int32, (PAN, BLK), 0)
    r_i = lax.broadcasted_iota(jnp.int32, (BLK, BLK), 0)
    c_i = lax.broadcasted_iota(jnp.int32, (BLK, BLK), 1)
    w_ref[...] = (r_i == c_i).astype(F32)

    def body(p, carry):
        x, *cols = carry
        base = pl.multiple_of(p * PAN, PAN)
        nxt = pl.multiple_of(jnp.minimum(base + PAN, BLK - PAN), PAN)
        fwd = w_ref[pl.ds(base, PAN), :]
        kw = fwd
        scale = jnp.zeros((PAN, BLK), F32)
        for j in range(PAN):
            d = row_of(cols[j], j)
            r = 1.0 / d
            f = cols[j] * r
            isj = sub == j
            for m in range(j + 1, PAN):
                b = row_of(cols[m], j)
                cols[m] = jnp.where(isj, b * r, cols[m] - f * b)
            b = row_of(x, j)
            x = jnp.where(isj, b * r, x - f * b)
            b = row_of(kw, j)
            kw = jnp.where(isj, b * r, kw - f * b)
            if j < PAN - 1:
                fwd = jnp.where(sub > j, fwd - f * row_of(fwd, j), fwd)
            scale = jnp.where(isj, lax.rsqrt(d), scale)
        m_ref[pl.ds(base, PAN), :] = fwd * scale
        xb = [row_of(x, m) for m in range(PAN)]
        kb = [row_of(kw, m) for m in range(PAN)]
        side(p)
        an = a_ref[pl.ds(nxt, PAN), :]
        xn = an - rows_sum([lanes_of(an, base + m) for m in range(PAN)], xb)
        new_cols = [lanes_of(xn, nxt + m) for m in range(PAN)]
        raw = carry[0]
        rh, rm = split(raw)
        rl = (raw - rh.astype(F32) - rm.astype(F32)).astype(BF)
        bb = jnp.concatenate([x, kw], axis=1)
        bh, bm = split(bb)
        bl = (bb - bh.astype(F32) - bm.astype(F32)).astype(BF)
        f32 = lambda v: v.astype(F32)
        left = jnp.concatenate([f32(v) for v in (rh, rh, rm, rm, rh, rl)], axis=0).astype(BF)
        right = jnp.concatenate([f32(v) for v in (bh, bm, bh, bm, bl, bh)], axis=0).astype(BF)
        upd = lax.dot_general(left, right, (((0,), (0,)), ((), ())), preferred_element_type=F32)
        a_ref[...] = a_ref[...] - upd[:, :BLK]
        w_ref[...] = w_ref[...] - upd[:, BLK:]
        return (xn, *new_cols)

    x0 = a_ref[0:PAN, :]
    lax.fori_loop(0, BLK // PAN, body, (x0, *[lanes_of(x0, m) for m in range(PAN)]))


MESH = pl.DeviceIdType.MESH
NB = 1024
NGROUPS = 16
NBLK = NB // BLK
TILES = NBLK * (NBLK + 1) // 2
ANY = pl.BlockSpec(memory_space=pltpu.HBM)


def tile_row(i, j):
    return (i * (i + 1) // 2 + j) * BLK


def place():
    band, coef = lax.axis_index("band"), lax.axis_index("coef")
    return band, coef, dict(z=band // 4, x=band % 4, y=coef // 2, core=coef % 2)


def peer_on(pos, dim, value):
    p = dict(pos)
    p[dim] = value
    return (p["z"] * 4 + p["x"], p["y"] * 2 + p["core"])


def send(src, dst, ssem, rsem, device):
    copy = pltpu.make_async_remote_copy(
        src_ref=src, dst_ref=dst, send_sem=ssem, recv_sem=rsem, device_id=device, device_id_type=MESH
    )
    copy.start()
    return copy


ORDERS = (("z", "x", "y"), ("x", "y", "z"), ("y", "z", "x"))
RING = 4
HALF = TILES * BLK // 2
PART = HALF // 3
Q1 = PART // RING
Q2 = Q1 // RING


def reduce_kernel(g_ref, o_ref, half_ref, b1_ref, a1_ref, b2_ref, b3_ref, csem, rsem, ssem):
    _, _, pos = place()
    partner = peer_on(pos, "core", 1 - pos["core"])
    peers = [partner] + [
        peer_on(pos, d, lax.rem(pos[d] + r, RING)) for d in ("z", "x", "y") for r in range(1, RING)
    ]
    barrier = pltpu.get_barrier_semaphore()
    for p in peers:
        pl.semaphore_signal(barrier, inc=1, device_id=p, device_id_type=MESH)
    pl.semaphore_wait(barrier, len(peers))

    core = pos["core"]
    mine = pl.multiple_of(core * HALF, PART)
    other = pl.multiple_of((1 - core) * HALF, PART)
    cs = [
        send(
            g_ref.at[pl.ds(pl.multiple_of(other + part * PART, PART), PART)],
            half_ref.at[part],
            csem.at[part],
            csem.at[3 + part],
            partner,
        )
        for part in range(3)
    ]
    c1 = []
    for part, (d1, _, _) in enumerate(ORDERS):
        cs[part].wait_recv()
        half_ref[part] = half_ref[part] + g_ref[pl.ds(pl.multiple_of(mine + part * PART, PART), PART), :]
        for r in (2, 1, 3):
            to = lax.rem(pos[d1] + r, RING)
            c1.append(
                send(
                    half_ref.at[part, pl.ds(pl.multiple_of(to * Q1, Q1), Q1)],
                    b1_ref.at[part, r - 1],
                    ssem.at[0, part, r - 1],
                    rsem.at[0, part, r - 1],
                    peer_on(pos, d1, to),
                )
            )
    c2 = []
    for part, (d1, d2, _) in enumerate(ORDERS):
        for c in c1[3 * part : 3 * part + 3]:
            c.wait_recv()
        own = half_ref[part, pl.ds(pl.multiple_of(pos[d1] * Q1, Q1), Q1), :]
        a1_ref[part] = own + b1_ref[part, 0] + (b1_ref[part, 1] + b1_ref[part, 2])
        for r in (2, 1, 3):
            to = lax.rem(pos[d2] + r, RING)
            c2.append(
                send(
                    a1_ref.at[part, pl.ds(pl.multiple_of(to * Q2, Q2), Q2)],
                    b2_ref.at[part, r - 1],
                    ssem.at[1, part, r - 1],
                    rsem.at[1, part, r - 1],
                    peer_on(pos, d2, to),
                )
            )
    c3 = []
    for part, (d1, d2, d3) in enumerate(ORDERS):
        for c in c2[3 * part : 3 * part + 3]:
            c.wait_recv()
        own = a1_ref[part, pl.ds(pl.multiple_of(pos[d2] * Q2, Q2), Q2), :]
        b3_ref[part, pos[d3]] = own + b2_ref[part, 0] + (b2_ref[part, 1] + b2_ref[part, 2])
        for r in (2, 1, 3):
            to = lax.rem(pos[d3] + r, RING)
            c3.append(
                send(
                    b3_ref.at[part, pos[d3]],
                    b3_ref.at[part, pos[d3]],
                    ssem.at[2, part, r - 1],
                    rsem.at[2, part, r - 1],
                    peer_on(pos, d3, to),
                )
            )
    c4 = []
    for part, (d1, d2, d3) in enumerate(ORDERS):
        for c in c3[3 * part : 3 * part + 3]:
            c.wait_recv()
        start = pl.multiple_of(mine + part * PART + pos[d1] * Q1 + pos[d2] * Q2, Q2)
        o_ref[pl.ds(start, Q2), :] = (b3_ref[part, 0] + b3_ref[part, 1]) + (b3_ref[part, 2] + b3_ref[part, 3])
        here = o_ref.at[pl.ds(start, Q2)]
        for r in (2, 1, 3):
            to = lax.rem(pos[d2] + r, RING)
            c4.append(send(here, here, ssem.at[3, part, r - 1], rsem.at[3, part, r - 1], peer_on(pos, d2, to)))
    c5 = []
    for part, (d1, d2, d3) in enumerate(ORDERS):
        for c in c4[3 * part : 3 * part + 3]:
            c.wait_recv()
        here = o_ref.at[pl.ds(pl.multiple_of(mine + part * PART + pos[d1] * Q1, Q2), Q1)]
        for r in (2, 1, 3):
            to = lax.rem(pos[d1] + r, RING)
            c5.append(send(here, here, ssem.at[4, part, r - 1], rsem.at[4, part, r - 1], peer_on(pos, d1, to)))
    c6 = []
    for part, (d1, d2, d3) in enumerate(ORDERS):
        for c in c5[3 * part : 3 * part + 3]:
            c.wait_recv()
        here = o_ref.at[pl.ds(pl.multiple_of(mine + part * PART, PART), PART)]
        c6.append(send(here, here, csem.at[6 + part], csem.at[9 + part], partner))
    for c in c6:
        c.wait_recv()
    for c in cs + c1 + c2 + c3 + c4 + c5 + c6:
        c.wait_send()


def reduce_all(g):
    return pl.pallas_call(
        reduce_kernel,
        out_shape=jax.ShapeDtypeStruct(g.shape, F32),
        in_specs=[pl.BlockSpec(memory_space=pltpu.VMEM)],
        out_specs=pl.BlockSpec(memory_space=pltpu.VMEM),
        scratch_shapes=[
            pltpu.VMEM((3, PART, BLK), F32),
            pltpu.VMEM((3, RING - 1, Q1, BLK), F32),
            pltpu.VMEM((3, Q1, BLK), F32),
            pltpu.VMEM((3, RING - 1, Q2, BLK), F32),
            pltpu.VMEM((3, RING, Q2, BLK), F32),
            pltpu.SemaphoreType.DMA((12,)),
            pltpu.SemaphoreType.DMA((5, 3, RING - 1)),
            pltpu.SemaphoreType.DMA((5, 3, RING - 1)),
        ],
        compiler_params=pltpu.CompilerParams(collective_id=0, has_side_effects=True, vmem_limit_bytes=60 * 2**20),
        name="reduce_all",
    )(g)


def solve_kernel(g_ref, c_ref, y_ref, a_ref, w_ref, m_ref, lh_ref, ll_ref, yh_ref, yl_ref, z_ref, csem, ysem):
    n = c_ref.shape[0]
    steps = n // BLK
    loads = []
    for k in range(steps):
        rows = pl.ds(k * BLK, BLK)
        loads.append(pltpu.make_async_copy(c_ref.at[rows], z_ref.at[rows], csem.at[k]))
        loads[-1].start()
    stores = []
    for k in range(steps):
        lo, hi = k * BLK, (k + 1) * BLK
        s = jnp.concatenate([g_ref[tile_row(i, k) : tile_row(i, k) + BLK, :] for i in range(k, steps)], axis=0)
        if k:
            s = s - dot3(lh_ref[lo:, :lo], ll_ref[lo:, :lo], lh_ref[lo:hi, :lo], ll_ref[lo:hi, :lo], NT)
        a_ref[...] = s[:BLK]
        loads[k].wait()
        wide = c_ref.shape[1] // (BLK // PAN)

        def side(p, lo=lo, hi=hi):
            if lo:
                cols = pl.ds(pl.multiple_of(p * wide, wide), wide)
                z_ref[lo:hi, cols] = z_ref[lo:hi, cols] - dot3(
                    lh_ref[lo:hi, :lo], ll_ref[lo:hi, :lo], yh_ref[:lo, cols], yl_ref[:lo, cols], NN
                )

        diag_inverse(a_ref, w_ref, m_ref, side)
        mh, ml = split(m_ref[...])
        if hi < n:
            sh, sl = split(s[BLK:])
            lkh, lkl = split(dot3(sh, sl, mh, ml, NT))
            lh_ref[hi:, lo:hi] = lkh
            ll_ref[hi:, lo:hi] = lkl
        zh, zl = split(z_ref[lo:hi, :])
        y = dot3(mh, ml, zh, zl, NN)
        z_ref[lo:hi, :] = y
        rows = pl.ds(lo, BLK)
        stores.append(pltpu.make_async_copy(z_ref.at[rows], y_ref.at[rows], ysem.at[k]))
        stores[-1].start()
        if hi < n:
            yh, yl = split(y)
            yh_ref[lo:hi, :] = yh
            yl_ref[lo:hi, :] = yl
    for c in stores:
        c.wait()


def solve(g, c):
    n, w = c.shape
    return pl.pallas_call(
        solve_kernel,
        out_shape=jax.ShapeDtypeStruct((n, w), F32),
        in_specs=[pl.BlockSpec(memory_space=pltpu.VMEM), ANY],
        out_specs=ANY,
        scratch_shapes=[pltpu.VMEM((BLK, BLK), F32)] * 3
        + [pltpu.VMEM((n, n), BF)] * 2
        + [pltpu.VMEM((n, w), BF)] * 2
        + [pltpu.VMEM((n, w), F32), pltpu.SemaphoreType.DMA((n // BLK,)), pltpu.SemaphoreType.DMA((n // BLK,))],
        compiler_params=pltpu.CompilerParams(vmem_limit_bytes=60 * 2**20),
        name="solve",
    )(g, c)


GB = 256


def gram_kernel(c_ref, g_ref, x_ref, h_ref, l_ref, sem):
    n = c_ref.shape[0]
    loads = {}
    for i in reversed(range(n // GB)):
        rows = pl.ds(i * GB, GB)
        loads[i] = pltpu.make_async_copy(c_ref.at[rows], x_ref.at[rows], sem.at[i])
        loads[i].start()
    def ready(i):
        rows = slice(i * GB, (i + 1) * GB)
        loads[i].wait()
        h_ref[rows, :], l_ref[rows, :] = split(x_ref[rows, :])

    last = n // GB - 1
    ready(last)
    for i in reversed(range(n // GB)):
        lo, e = i * GB, (i + 1) * GB
        if i:
            ready(i - 1)
        g = dot3(h_ref[lo:, :], l_ref[lo:, :], h_ref[lo:e, :], l_ref[lo:e, :], NT)
        for bj in range(lo // BLK, e // BLK):
            for bi in range(bj, n // BLK):
                t = tile_row(bi, bj)
                r, q = bi * BLK - lo, bj * BLK - lo
                g_ref[t : t + BLK, :] = g[r : r + BLK, q : q + BLK]


def gram(c):
    n, w = c.shape
    return pl.pallas_call(
        gram_kernel,
        out_shape=jax.ShapeDtypeStruct((TILES * BLK, BLK), F32),
        in_specs=[ANY],
        out_specs=pl.BlockSpec(memory_space=pltpu.VMEM),
        scratch_shapes=[
            pltpu.VMEM((n, w), F32),
            pltpu.VMEM((n, w), BF),
            pltpu.VMEM((n, w), BF),
            pltpu.SemaphoreType.DMA((n // GB,)),
        ],
        compiler_params=pltpu.CompilerParams(vmem_limit_bytes=60 * 2**20),
        name="gram",
    )(c)


HR = 32


def ring_kernel(to_rows, greet, side, done, c_ref, o_ref, src_ref, land_ref, b1_ref, r1_ref, r2_ref,
                lsem, osem, s1, v1, sr1, vr1, sf1, s2, v2, sr2, vr2, sf2, qsem):
    band, coef, pos = place()
    part = 2048
    bands = 64
    dims = (("z", "x"), ("x", "z"))

    def who(h, a, b):
        d1, d2 = dims[h]
        p = dict(pos)
        p[d1] = lax.rem(pos[d1] + a + RING, RING)
        p[d2] = lax.rem(pos[d2] + b + RING, RING)
        return p["z"] * 4 + p["x"]

    def wide(h, b):
        return (pl.ds(h * HR, HR), pl.ds(pl.multiple_of(b * part, part), part))

    def tall(h, b):
        return (pl.ds(pl.multiple_of(b * bands + h * HR, HR), HR), slice(None))

    far = tall if to_rows else wide

    def cell(h, b):
        return (b, pl.ds(h * HR, HR))

    loads = {}
    for a in range(RING):
        for b in range(RING):
            d = who(0, a, b)
            at = (slice(None), pl.ds(pl.multiple_of(d * part, part), part)) if to_rows else (
                pl.ds(pl.multiple_of(d * bands, bands), bands), slice(None))
            loads[a, b] = pltpu.make_async_copy(c_ref.at[at], src_ref.at[d], lsem.at[a, b])
    order = [(2, 1), (1, 2), (2, 3), (3, 2), (2, 2), (2, 0), (0, 2)]
    order += [k for k in loads if k not in order and k != (0, 0)] + [(0, 0)]
    for k in order:
        loads[k].start()
    peers = greet(band, coef) if greet else [
        (who(h, s, 0), coef) for h in range(2) for s in (1, -1)
    ]
    barrier = pltpu.get_barrier_semaphore()
    for p in peers:
        pl.semaphore_signal(barrier, inc=1, device_id=p, device_id_type=MESH)
    pl.semaphore_wait(barrier, len(peers))

    ready = set()

    def src(h, a, b):
        k = (a, b) if h == 0 else (b, a)
        if k not in ready:
            loads[k].wait()
            ready.add(k)
        return src_ref.at[cell(h, who(h, a, b))]

    sent = []

    def go(*args):
        sent.append(send(*args))
        return sent[-1]

    SIGN = (1, -1)
    VIA1 = ((2, 1), (3, 0))
    VIA2 = ((0, 1), (3, 2))
    rel1 = {}
    for i in range(2):
        for h in range(2):
            for g in range(2):
                q = VIA1[g][i]
                rel1[h, g, i] = go(src(h, 2, q), r1_ref.at[h, g, i], sr1.at[h, g, i], vr1.at[h, g, i],
                                   (who(h, SIGN[g], 0), coef))
    dir1 = {}
    for q in (2, 1, 3, 0):
        for h in range(2):
            for g in range(2):
                r = 1 if g == 0 else 3
                dir1[h, r, q] = go(src(h, r, q), b1_ref.at[h, r - 1, q], s1.at[h, r - 1, q], v1.at[h, r - 1, q],
                                   (who(h, SIGN[g], 0), coef))
    side(0)
    for i in range(2):
        for h in range(2):
            for g in range(2):
                q = VIA1[g][i]
                rel1[h, g, i].wait_recv()
                dir1[h, 2, q] = go(r1_ref.at[h, g, i], b1_ref.at[h, 1, q], sf1.at[h, g, i], v1.at[h, 1, q],
                                   (who(h, SIGN[g], 0), coef))
    rel2, fin, outs = {}, {}, []

    def second(h, r, q):
        block = src(h, 0, q) if r == 0 else b1_ref.at[h, r - 1, q]
        if q == 0:
            at = far(h, who(h, -r, 0))
            outs.append(pltpu.make_async_copy(block, o_ref.at[at], qsem.at[h, r]))
            outs[-1].start()
        elif q == 2:
            g = 0 if r in VIA2[0] else 1
            i = VIA2[g].index(r)
            rel2[h, g, i] = go(block, r2_ref.at[h, g, i], sr2.at[h, g, i], vr2.at[h, g, i],
                               (who(h, 0, SIGN[g]), coef))
        else:
            at = land_ref.at[cell(h, who(h, -r, 0))]
            fin[h, r, q] = go(block, at, s2.at[h, r, q - 1], v2.at[h, r, q - 1],
                              (who(h, 0, 1 if q == 1 else -1), coef))

    for q in (2, 1, 3, 0):
        for h in range(2):
            second(h, 0, q)
    side(1)
    for q in (2, 1, 3, 0):
        for r in (1, 3):
            for h in range(2):
                dir1[h, r, q].wait_recv()
                second(h, r, q)
        side(2)
    for n, q in enumerate((2, 3, 1, 0)):
        for h in range(2):
            dir1[h, 2, q].wait_recv()
            second(h, 2, q)
        if n % 2:
            side(3)
    for i in range(2):
        for h in range(2):
            for g in range(2):
                r = VIA2[g][i]
                rel2[h, g, i].wait_recv()
                at = land_ref.at[cell(h, who(h, -r, -SIGN[g]))]
                fin[h, r, 2] = go(r2_ref.at[h, g, i], at, sf2.at[h, g, i], v2.at[h, r, 1],
                                  (who(h, 0, SIGN[g]), coef))
    side(4)
    for r in range(RING):
        for h in range(2):
            b = who(h, -r, 0)
            done(h, b, src_ref.at[cell(h, band)] if r == 0 else b1_ref.at[h, r - 1, 0])
    for r in (0, 1, 3, 2):
        for q in (1, 3, 2):
            for h in range(2):
                fin[h, r, q].wait_recv()
                b = who(h, -r, -q)
                done(h, b, land_ref.at[cell(h, b)])
                outs.append(
                    pltpu.make_async_copy(land_ref.at[cell(h, b)], o_ref.at[far(h, b)], osem.at[h, r, q - 1])
                )
                outs[-1].start()
    for c in sent:
        c.wait_send()
    return outs


RING_SCRATCH = [
    pltpu.VMEM((16, 64, 2048), F32),
    pltpu.VMEM((16, 64, 2048), F32),
    pltpu.VMEM((2, 3, 4, HR, 2048), F32),
    pltpu.VMEM((2, 2, 2, HR, 2048), F32),
    pltpu.VMEM((2, 2, 2, HR, 2048), F32),
] + [
    pltpu.SemaphoreType.DMA(s)
    for s in (
        (4, 4), (2, 4, 3), (2, 3, 4), (2, 3, 4), (2, 2, 2), (2, 2, 2), (2, 2, 2),
        (2, 4, 3), (2, 4, 3), (2, 2, 2), (2, 2, 2), (2, 2, 2), (2, 4),
    )
]


def exchange(slots, index, peers, ssem, rsem):
    here = slots.at[index]
    copies = [send(here, here, ssem.at[r], rsem.at[r], p) for r, p in enumerate(peers)]
    for c in copies:
        c.wait_recv()
    return copies


CH = 2048


def spread_kernel(idx_ref, c_ref, o_ref, inv_ref, acc_ref, *scratch):
    tall_, lanes_ = idx_ref.shape
    group = 16

    def side(stage):
        if stage:
            return
        acc_ref[...] = jnp.zeros_like(acc_ref)
        lane = lax.broadcasted_iota(jnp.int32, (BLK, lanes_), 1)
        his = lax.broadcasted_iota(jnp.int32, (tall_, lanes_), 0)
        los = lax.broadcasted_iota(jnp.int32, (BLK, lanes_), 0)

        def body(c, _):
            hots, boths = [], []
            for u in range(group):
                row = c * group + u
                idx = idx_ref[pl.ds(row, 1), :]
                hots.append(jnp.where(his == (idx >> 7), 1.0, 0.0).astype(BF))
                low = los == (idx & 127)
                top = jnp.where(low, jnp.full((BLK, lanes_), row, jnp.int32).astype(F32), 0.0)
                bot = jnp.where(low, lane.astype(F32), 0.0)
                boths.append(jnp.concatenate([top, bot], axis=0).astype(BF))
            acc_ref[...] += lax.dot_general(
                jnp.concatenate(hots, axis=1),
                jnp.concatenate(boths, axis=1),
                (NT, ((), ())),
                preferred_element_type=F32,
            )
            return 0

        lax.fori_loop(0, tall_ // group, body, 0)
        inv_ref[...] = acc_ref[:, :BLK].astype(jnp.int32) * BLK + acc_ref[:, BLK:].astype(jnp.int32)

    outs = ring_kernel(True, None, side, lambda *a: None, c_ref, o_ref, *scratch)
    for c in outs:
        c.wait()


def spread(idx, c):
    a, b = c.shape
    vm = pl.BlockSpec(memory_space=pltpu.VMEM)
    return pl.pallas_call(
        spread_kernel,
        out_shape=(
            jax.ShapeDtypeStruct((a * 16, b // 16), F32),
            jax.ShapeDtypeStruct((b // BLK, BLK), jnp.int32),
        ),
        in_specs=[vm, ANY],
        out_specs=(ANY, vm),
        scratch_shapes=[pltpu.VMEM((b // BLK, 2 * BLK), F32), *RING_SCRATCH],
        compiler_params=pltpu.CompilerParams(
            collective_id=2, has_side_effects=True, vmem_limit_bytes=60 * 2**20
        ),
        name="spread",
    )(idx.reshape(b // BLK, BLK), c)


STOPS = (0, 2, 4, 6, 8, 10, 12, 14, 16)


def collect_kernel(inv_ref, y_ref, q_ref, grp_ref, o_ref, res_ref, tot_ref,
                   want_ref, rows_ref, got_ref, acc_ref, sq_ref, gr_ref, isem, s2, r2, s3, r3, *scratch):
    band, coef, _ = place()
    nband, ncoef = gr_ref.shape[0], sq_ref.shape[0]
    bands, width = q_ref.shape
    n = width // CH
    bpeers = [(lax.rem(band + r, nband), coef) for r in range(1, nband)]
    cpeers = [(band, lax.rem(coef + r, ncoef)) for r in range(1, ncoef)]

    def columns(s):
        return pl.ds(pl.multiple_of(s * CH, CH), CH)

    def load(s):
        return pltpu.make_async_copy(q_ref.at[:, columns(s)], want_ref.at[:, columns(s)], isem.at[s])

    def turn(s, _):
        load(s).wait()
        rows_ref[columns(s), :] = want_ref[:, columns(s)].T
        return 0

    def gather(s, _):
        def body(i, _):
            at = i * 16
            for u in range(16):
                got_ref[pl.ds(at + u, 1), :] = rows_ref[pl.ds(inv_ref[s * CH + at + u], 1), :]
            return 0

        lax.fori_loop(0, CH // 16, body, 0)
        want_ref[:, columns(s)] = got_ref[...].T
        return 0

    calls = []

    def side(stage):
        if stage == 0:
            acc_ref[...] = jnp.zeros_like(acc_ref)
            for s in range(n):
                load(s).start()
            lax.fori_loop(0, n, turn, 0)
            return
        k = len(calls)
        calls.append(stage)
        last = STOPS[k + 1] if stage < 4 else n
        lax.fori_loop(STOPS[k], last, gather, 0)

    def done(h, b, block):
        step = 4 * BLK

        def body(i, acc):
            at = pl.multiple_of(i * step, step)
            d = block[:, pl.ds(at, step)] - want_ref[pl.ds(h * HR, HR), pl.ds(pl.multiple_of(b * CH + at, step), step)]
            d = d * d
            return acc + ((d[:, :BLK] + d[:, BLK : 2 * BLK]) + (d[:, 2 * BLK : 3 * BLK] + d[:, 3 * BLK :]))

        acc_ref[h] = lax.fori_loop(0, CH // step, body, acc_ref[h])

    outs = ring_kernel(False, lambda *a: bpeers + cpeers, side, done, y_ref, o_ref, *scratch)

    row = lax.broadcasted_iota(jnp.int32, (bands, BLK), 0)
    lane = lax.broadcasted_iota(jnp.int32, (bands, BLK), 1)
    total = jnp.sum(jnp.concatenate([acc_ref[0], acc_ref[1]], axis=0), axis=1, keepdims=True)
    line = jnp.sum(jnp.where(row == lane, total, 0.0), axis=0, keepdims=True)
    sq_ref[coef] = jnp.broadcast_to(line, (8, BLK))
    c2 = exchange(sq_ref, coef, cpeers, s2, r2)
    tot = sq_ref[0]
    for q in range(1, ncoef):
        tot = tot + sq_ref[q]
    res = jnp.sqrt(tot + 1e-06)
    res_ref[...] = res
    g16 = lax.broadcasted_iota(jnp.int32, (NGROUPS, BLK), 0)
    gr_ref[band] = jnp.where(g16 == grp_ref[0:1, :], res[0:1, :], 0.0)
    c3 = exchange(gr_ref, band, bpeers, s3, r3)
    g = gr_ref[0]
    for q in range(1, nband):
        g = g + gr_ref[q]
    row = lax.broadcasted_iota(jnp.int32, (NGROUPS, BLK), 0)
    lane = lax.broadcasted_iota(jnp.int32, (NGROUPS, BLK), 1)
    g = jnp.sum(g, axis=1, keepdims=True) * (NGROUPS / NB)
    tot_ref[...] = jnp.broadcast_to(jnp.sum(jnp.where(row == lane, g, 0.0), axis=0, keepdims=True), (8, BLK))
    for c in outs:
        c.wait()
    for c in c2 + c3:
        c.wait_send()


def collect(inv, y, q, grp):
    bands, width = q.shape
    vm = pl.BlockSpec(memory_space=pltpu.VMEM)
    nband, ncoef = lax.axis_size("band"), lax.axis_size("coef")
    dma = pltpu.SemaphoreType.DMA
    return pl.pallas_call(
        collect_kernel,
        out_shape=(
            jax.ShapeDtypeStruct((bands, width), F32),
            jax.ShapeDtypeStruct((8, BLK), F32),
            jax.ShapeDtypeStruct((8, BLK), F32),
        ),
        in_specs=[pl.BlockSpec(memory_space=pltpu.SMEM), ANY, ANY, vm],
        out_specs=(ANY, vm, vm),
        scratch_shapes=[
            pltpu.VMEM((bands, width), F32),
            pltpu.VMEM((width, bands), F32),
            pltpu.VMEM((CH, bands), F32),
            pltpu.VMEM((2, HR, BLK), F32),
            pltpu.VMEM((ncoef, 8, BLK), F32),
            pltpu.VMEM((nband, NGROUPS, BLK), F32),
            dma((width // CH,)),
            dma((ncoef - 1,)),
            dma((ncoef - 1,)),
            dma((nband - 1,)),
            dma((nband - 1,)),
            *RING_SCRATCH,
        ],
        compiler_params=pltpu.CompilerParams(
            collective_id=3, has_side_effects=True, vmem_limit_bytes=60 * 2**20
        ),
        name="collect",
    )(inv.reshape(width), y, q, grp)


def finish_kernel(raw_ref, res_ref, tot_ref, o_ref, band_ref, group_ref, buf_ref, isem, osem):
    n = raw_ref.shape[0] // 8
    ins = [pltpu.make_async_copy(raw_ref.at[pl.ds(8 * s, 8)], buf_ref.at[s], isem.at[s]) for s in range(n)]
    outs = [pltpu.make_async_copy(buf_ref.at[s], o_ref.at[pl.ds(8 * s, 8)], osem.at[s]) for s in range(n)]
    for c in ins:
        c.start()
    band_ref[...] = res_ref[0, : band_ref.shape[0]]
    group_ref[...] = tot_ref[0, : group_ref.shape[0]]
    for a, b in zip(ins, outs):
        a.wait()
        b.start()
    for c in outs:
        c.wait()


def finish(raw, res, tot):
    bands, width = raw.shape
    vm = pl.BlockSpec(memory_space=pltpu.VMEM)
    return pl.pallas_call(
        finish_kernel,
        out_shape=(
            jax.ShapeDtypeStruct((bands, width), F32),
            jax.ShapeDtypeStruct((bands,), F32),
            jax.ShapeDtypeStruct((NGROUPS,), F32),
        ),
        in_specs=[ANY, vm, vm],
        out_specs=(ANY, vm, vm),
        scratch_shapes=[
            pltpu.VMEM((bands // 8, 8, width), F32),
            pltpu.SemaphoreType.DMA((bands // 8,)),
            pltpu.SemaphoreType.DMA((bands // 8,)),
        ],
        compiler_params=pltpu.CompilerParams(vmem_limit_bytes=60 * 2**20),
        name="finish",
    )(raw, res, tot)


def local(coeffs, ref_block, index_map, band_group):
    bands, _ = coeffs.shape
    columns, inv = spread(index_map, coeffs)
    margin = reduce_all(gram(columns))
    groups = jnp.broadcast_to(jnp.pad(band_group, (0, BLK - bands), constant_values=-1), (8, BLK))
    return finish(*collect(inv, solve(margin, columns), ref_block, groups))


def solution(mesh):
    return jax.shard_map(
        local,
        mesh=mesh,
        in_specs=(P("band", "coef"), P("band", "coef"), P("coef"), P("band")),
        out_specs=(P("band", "coef"), P("band"), P()),
        check_vma=False,
    )
```
